256 devices in a mesh: rows: 32 (over y, x, core), cols: 8 (over z).
Axes of the slice: x: 4, y: 4, z: 8, core: 2. Of those that a mesh axis runs over, the one named last changes fastest.
Arguments:
- one_query: float32 [8192, 8192], P('rows', 'cols'), may hold values from -0.125 to 0.125
- other_query: float32 [8192, 8192], P('rows', 'cols'), may hold values from -0.0625 to 0.0625
- one_key: float32 [8192, 512], P('rows', 'cols'), may hold values from -0.125 to 0.125
- other_key: float32 [8192, 512], P('rows', 'cols'), may hold values from -0.0625 to 0.0625
- one_value: float32 [8192, 512], P('rows', 'cols'), may hold values from -0.125 to 0.125
- other_value: float32 [8192, 512], P('rows', 'cols'), may hold values from -0.0625 to 0.0625
- mix_share: float32 [8192], P('rows'), may hold values from 0.2 to 0.8
- norm_gain: float32 [8192], P('rows'), may hold values from 0.25 to 1.75
Outputs:
- serve_query: bfloat16 [8192, 8192], P(None, 'cols')
- serve_key: bfloat16 [8192, 512], P(None, 'cols')
- serve_value: bfloat16 [8192, 512], P(None, 'cols')
- scale_query: float32 [8192], P('cols')
- scale_key: float32 [512], P('cols')
- scale_value: float32 [512], P('cols')
The draws below stay inside these ranges and needn't reach their ends.
All inputs are finite; a program needn't handle non-finite values. Where the reference program divides by a largest or mean magnitude, that divisor is 1e-20 or more.
Results may differ from the reference program's by a relative error of at most 0.001.
Values may be sent and summed in bfloat16 or wider, within the bound.
A program may use at most 128 MiB of HBM per device.

```python
import jax
import jax.numpy as jnp

D_MODEL = 8192
Q_DIM = 8192
KV_DIM = 512


def strengthened(drawn, stream_key, source, target, parts, factor):
    owner, partner = [(jnp.arange(drawn.shape[dim]) // (drawn.shape[dim] // parts)).reshape([-1 if axis == dim else 1 for axis in range(drawn.ndim)]) for dim in (source, target)]
    chosen = jax.random.permutation(stream_key, parts)[partner]
    strong = (owner == chosen) | (owner == (partner + parts // 2) % parts)
    return jnp.where(strong, factor * drawn, drawn)


def block_levels(own_key, extent, cuts, low, high):
    level, own = 1.0, jax.random.fold_in(own_key, 6)
    for axis_at, parts in cuts:
        steps = jnp.exp(jax.random.uniform(jax.random.fold_in(own, axis_at), (parts,), jnp.float32, low / len(cuts), high / len(cuts)))
        level = level * jnp.repeat(steps, extent[axis_at] // parts).reshape([-1 if axis == axis_at else 1 for axis in range(len(extent))])
    return level


def gaussian(own_key, extent, width, reach, shards=(), dtype=jnp.bfloat16):
    drawn = width * jax.random.normal(own_key, extent, jnp.float32)
    if shards:
        drawn = drawn * block_levels(own_key, extent, shards, -0.22, 0.18)
    return jnp.clip(drawn, -reach, reach).astype(dtype)


def gaussian_with(own_key, dims, deviation, reach, cuts, heavy, dtype=jnp.bfloat16):
    drawn = deviation * jax.random.normal(own_key, dims, jnp.float32)
    if cuts:
        drawn = drawn * block_levels(own_key, dims, cuts, -0.22, 0.18)
    return jnp.clip(strengthened(drawn, jax.random.fold_in(own_key, 3), *heavy), -reach, reach).astype(dtype)


def setup_inputs(seed: int = 0) -> dict:
    streams_of = jax.random.split(jax.random.key(seed), 9)
    one_query = gaussian_with(streams_of[0], (D_MODEL, Q_DIM), D_MODEL ** -0.5, 0.125, ((0, 32), (1, 8)), (0, 1, 32, 2.75), jnp.float32)
    other_query = gaussian(streams_of[1], (D_MODEL, Q_DIM), D_MODEL ** -0.5, 0.0625, ((0, 32), (1, 8)), jnp.float32)
    one_key = gaussian_with(streams_of[2], (D_MODEL, KV_DIM), D_MODEL ** -0.5, 0.125, ((0, 32), (1, 8)), (0, 1, 32, 2.75), jnp.float32)
    other_key = gaussian(streams_of[3], (D_MODEL, KV_DIM), D_MODEL ** -0.5, 0.0625, ((0, 32), (1, 8)), jnp.float32)
    one_value = gaussian_with(streams_of[4], (D_MODEL, KV_DIM), D_MODEL ** -0.5, 0.125, ((0, 32), (1, 8)), (0, 1, 32, 2.75), jnp.float32)
    other_value = gaussian(streams_of[5], (D_MODEL, KV_DIM), D_MODEL ** -0.5, 0.0625, ((0, 32), (1, 8)), jnp.float32)
    mix_share = jnp.clip(0.2 + 0.6 * jax.random.uniform(streams_of[6], (D_MODEL,), jnp.float32) ** block_levels(streams_of[6], (D_MODEL,), ((0, 32),), -0.2, 0.2), 0.2, 0.8)
    norm_gain = jnp.clip(1.0 + 0.15 * jax.random.normal(streams_of[7], (D_MODEL,), jnp.float32), 0.25, 1.75)
    return dict(one_query=one_query, other_query=other_query, one_key=one_key, other_key=other_key, one_value=one_value, other_value=other_value, mix_share=mix_share, norm_gain=norm_gain)


def reference(one_query, other_query, one_key, other_key, one_value, other_value, mix_share, norm_gain):
    fresh_query = mix_share[:, None] * one_query + (1.0 - mix_share[:, None]) * other_query
    fresh_key = mix_share[:, None] * one_key + (1.0 - mix_share[:, None]) * other_key
    fresh_value = mix_share[:, None] * one_value + (1.0 - mix_share[:, None]) * other_value
    fresh_gained_query = fresh_query * norm_gain[:, None]
    fresh_gained_key = fresh_key * norm_gain[:, None]
    fresh_gained_value = fresh_value * norm_gain[:, None]
    scale_query = jnp.sum(jnp.abs(fresh_gained_query), axis=0) / D_MODEL
    serve_query = (fresh_gained_query / scale_query).astype(jnp.bfloat16)
    scale_key = jnp.sum(jnp.abs(fresh_gained_key), axis=0) / D_MODEL
    serve_key = (fresh_gained_key / scale_key).astype(jnp.bfloat16)
    scale_value = jnp.sum(jnp.abs(fresh_gained_value), axis=0) / D_MODEL
    serve_value = (fresh_gained_value / scale_value).astype(jnp.bfloat16)
    return serve_query, serve_key, serve_value, scale_query, scale_key, scale_value
```

```python
import functools

import jax
import jax.numpy as jnp
from jax import lax
from jax.experimental import pallas as pl
from jax.experimental.pallas import tpu as pltpu
from jax.sharding import PartitionSpec as P

D_MODEL = 8192
MESH = pl.DeviceIdType.MESH
NX, NY, NC = 4, 4, 2
UNIT = 64

PLUS_X = (
    (0, 0, 0), (0, 0, 1), (0, 0, 2), (-1, 0, 0), (0, 0, 3), (0, -1, 2), (0, 1, 2), (-1, 0, 2),
    (0, 2, 2), (-1, -1, 2), (0, -1, 3), (-1, 1, 2), (0, 1, 3), (-1, 2, 2), (0, 2, 3),
)


def mirrored(items):
    return tuple((-dx, -dy, q ^ 1) for dx, dy, q in items)


def turned(items):
    return tuple((dy, dx, q ^ 2) for dx, dy, q in items)


LINKS = (
    (1, 0, PLUS_X),
    (-1, 0, mirrored(PLUS_X)),
    (0, 1, turned(PLUS_X)),
    (0, -1, mirrored(turned(PLUS_X))),
)


def received(link, slot):
    sx, sy, items = LINKS[link]
    dx, dy, q = items[slot]
    return ((dx - sx) % NX, (dy - sy) % NY, q)


STEPS = len(PLUS_X)
ARRIVAL = {received(link, slot): slot for link in range(4) for slot in range(STEPS)}


def due(link, slot):
    dx, dy, q = LINKS[link][2][slot]
    return -1 if (dx, dy) == (0, 0) else ARRIVAL[(dx % NX, dy % NY, q)]


def gather_kernel(
    one_q, other_q, one_k, other_k, one_v, other_v, mix, gain,
    full, total,
    in_one_q, in_other_q, in_one_kv, in_other_kv, in_mix, in_gain,
    gained, part, row_sums, mid, col_sums,
    load_sem, row_send, row_recv, col_send, col_recv, send_sem, recv_sem, pair_recv,
):
    me = lax.axis_index("rows")
    core = lax.rem(me, NC)
    chip = lax.div(me, NC)
    x = lax.rem(chip, NX)
    y = lax.div(chip, NX)

    def at(dx, dy):
        return lax.rem(y + dy % NY, NY) * NX + lax.rem(x + dx % NX, NX)

    def device(dx, dy, c):
        return {"rows": at(dx, dy) * NC + c}

    row_peers = [(1, 0, core), (3, 0, core), (2, 0, core), (1, 0, 1 - core), (3, 0, 1 - core), (2, 0, 1 - core), (0, 0, 1 - core)]
    col_peers = [(0, 1, core), (0, 3, core), (0, 2, core)]
    barrier = pltpu.get_barrier_semaphore()
    for peer in row_peers + col_peers:
        pl.semaphore_signal(barrier, inc=1, device_id=device(*peer), device_id_type=MESH)

    loads = [
        pltpu.make_async_copy(mix, in_mix, load_sem.at[0]),
        pltpu.make_async_copy(gain, in_gain, load_sem.at[1]),
        pltpu.make_async_copy(one_k, in_one_kv.at[pl.ds(0, 64)], load_sem.at[2]),
        pltpu.make_async_copy(one_v, in_one_kv.at[pl.ds(64, 64)], load_sem.at[3]),
        pltpu.make_async_copy(other_k, in_other_kv.at[pl.ds(0, 64)], load_sem.at[4]),
        pltpu.make_async_copy(other_v, in_other_kv.at[pl.ds(64, 64)], load_sem.at[5]),
    ]
    halves = []
    for h in range(2):
        rows = pl.ds(128 * h, 128)
        halves.append([
            pltpu.make_async_copy(one_q.at[rows], in_one_q.at[rows], load_sem.at[6 + 2 * h]),
            pltpu.make_async_copy(other_q.at[rows], in_other_q.at[rows], load_sem.at[7 + 2 * h]),
        ])
    for copy in loads + halves[0] + halves[1]:
        copy.start()
    for copy in loads:
        copy.wait()

    m, g = in_mix[...], in_gain[...]
    kv = (m * in_one_kv[...] + (1.0 - m) * in_other_kv[...]) * g
    kv_sum = jnp.sum(jnp.abs(kv), axis=1, keepdims=True)
    gained[pl.ds(0, 128), pl.ds(1024, 128)] = kv[:, :128]
    gained[pl.ds(128, 128), pl.ds(1024, 128)] = kv[:, 128:]
    part[:, pl.ds(1024, 128)] = jnp.transpose(jnp.broadcast_to(kv_sum, (128, 128)))[:1]

    sums = jnp.zeros((8, 1024), jnp.float32)
    for h in range(2):
        for copy in halves[h]:
            copy.wait()
        m_rows = jnp.transpose(jnp.broadcast_to(m[:, 128 * h : 128 * h + 128], (128, 128)))
        g_rows = jnp.transpose(jnp.broadcast_to(g[:, 128 * h : 128 * h + 128], (128, 128)))
        for t in range(16):
            rows = pl.ds(128 * h + 8 * t, 8)
            mt = jnp.concatenate([m_rows[8 * t : 8 * t + 8]] * 8, axis=1)
            gt = jnp.concatenate([g_rows[8 * t : 8 * t + 8]] * 8, axis=1)
            value = (mt * in_one_q[rows, :] + (1.0 - mt) * in_other_q[rows, :]) * gt
            gained[rows, pl.ds(0, 1024)] = value
            sums = sums + jnp.abs(value)
    part[:, pl.ds(0, 1024)] = jnp.sum(sums, axis=0, keepdims=True)

    pl.semaphore_wait(barrier, len(row_peers) + len(col_peers))
    own = x * NC + core
    copies = []
    for i, (dx, dy, c) in enumerate(row_peers):
        copies.append(pltpu.make_async_remote_copy(
            src_ref=part, dst_ref=row_sums.at[own], send_sem=row_send.at[i],
            recv_sem=row_recv.at[i], device_id=device(dx, dy, c), device_id_type=MESH,
        ))
        copies[-1].start()
    row_sums[own] = part[...]
    for copy in copies:
        copy.wait()
    subtotal = row_sums[0]
    for i in range(1, NX * NC):
        subtotal = subtotal + row_sums[i]
    mid[...] = subtotal
    copies = []
    for i, (dx, dy, c) in enumerate(col_peers):
        copies.append(pltpu.make_async_remote_copy(
            src_ref=mid, dst_ref=col_sums.at[y], send_sem=col_send.at[i],
            recv_sem=col_recv.at[i], device_id=device(dx, dy, c), device_id_type=MESH,
        ))
        copies[-1].start()
    col_sums[y] = mid[...]
    for copy in copies:
        copy.wait()
    subtotal = col_sums[0]
    for i in range(1, NY):
        subtotal = subtotal + col_sums[i]
    scale = subtotal / D_MODEL
    total[...] = scale
    inverse = 1.0 / scale
    inverse_kv = jnp.transpose(jnp.broadcast_to(inverse[:, 1024:], (128, 128)))

    def rows_of(dx, dy, q):
        return pl.ds(pl.multiple_of((core * NX * NY + at(dx, dy)) * 256 + q * UNIT, UNIT), UNIT)

    def send(link, slot):
        sx, sy, items = LINKS[link]
        rows = rows_of(*items[slot])
        pltpu.make_async_remote_copy(
            src_ref=full.at[rows], dst_ref=full.at[rows], send_sem=send_sem,
            recv_sem=recv_sem.at[link, slot], device_id=device(sx, sy, core), device_id_type=MESH,
        ).start()

    def share(dx, dy, q):
        rows = rows_of(dx, dy, q)
        pltpu.make_async_remote_copy(
            src_ref=full.at[rows], dst_ref=full.at[rows], send_sem=send_sem,
            recv_sem=pair_recv, device_id=device(0, 0, 1 - core), device_id_type=MESH,
        ).start()

    for q in range(4):
        rows = pl.ds(q * UNIT, UNIT)
        dst = rows_of(0, 0, q)
        full[dst, pl.ds(0, 1024)] = (gained[rows, pl.ds(0, 1024)] * inverse[:, :1024]).astype(jnp.bfloat16)
        half = (q % 2) * UNIT
        full[dst, pl.ds(1024, 128)] = (gained[rows, pl.ds(1024, 128)] * inverse_kv[half : half + UNIT]).astype(jnp.bfloat16)

    sent = [0, 0, 0, 0]
    for slot in range(-1, STEPS):
        if slot >= 0:
            for link in range(4):
                dx, dy, q = received(link, slot)
                rows = rows_of(dx, dy, q)
                pltpu.make_async_remote_copy(
                    src_ref=full.at[rows], dst_ref=full.at[rows], send_sem=send_sem,
                    recv_sem=recv_sem.at[link, slot], device_id=device(0, 0, 1 - core), device_id_type=MESH,
                ).wait_recv()
                share(dx, dy, q)
        for link in range(4):
            while sent[link] < STEPS and due(link, sent[link]) <= slot:
                send(link, sent[link])
                sent[link] += 1
        if slot == -1:
            for q in range(4):
                share(0, 0, q)

    other = pl.ds(pl.multiple_of((1 - core) * 4096, 4096), 4096)
    pltpu.make_async_copy(full.at[other], full.at[other], pair_recv).wait()
    everything = pl.ds(0, (4 * STEPS + 64) * UNIT)
    pltpu.make_async_copy(full.at[everything], full.at[everything], send_sem).wait()


def write_kernel(full, total, query, key, value, scale_q, scale_k, scale_v, sem):
    copies = [
        pltpu.make_async_copy(total.at[:, pl.ds(0, 1024)], scale_q, sem.at[0]),
    ]
    n = 1
    for c in range(NC):
        for p in range(NX * NY):
            src, dst = (c * NX * NY + p) * 256, (p * NC + c) * 256
            copies.append(pltpu.make_async_copy(full.at[pl.ds(src, 256), pl.ds(0, 1024)], query.at[pl.ds(dst, 256)], sem.at[n]))
            n += 1
            for q in range(4):
                out = (key, value)[q % 2]
                copies.append(pltpu.make_async_copy(
                    full.at[pl.ds(src + q * UNIT, UNIT), pl.ds(1024, 128)],
                    out.at[:, pl.ds(dst + 128 * (q // 2), 128)],
                    sem.at[n],
                ))
                n += 1
    for copy in copies:
        copy.start()
    scale_k[...] = total[:, 1024:1088]
    scale_v[...] = total[:, 1088:1152]
    for copy in copies:
        copy.wait()


def local(one_query, other_query, one_key, other_key, one_value, other_value, mix_share, norm_gain):
    hbm = pl.BlockSpec(memory_space=pltpu.HBM)
    vmem = pl.BlockSpec(memory_space=pltpu.VMEM)
    f32, bf16 = jnp.float32, jnp.bfloat16
    full, total = pl.pallas_call(
        gather_kernel,
        out_shape=(pltpu.VMEM((8192, 1152), bf16), pltpu.VMEM((1, 1152), f32)),
        in_specs=[hbm] * 8,
        out_specs=(vmem, vmem),
        scratch_shapes=[
            pltpu.VMEM((256, 1024), f32),
            pltpu.VMEM((256, 1024), f32),
            pltpu.VMEM((128, 256), f32),
            pltpu.VMEM((128, 256), f32),
            pltpu.VMEM((1, 256), f32),
            pltpu.VMEM((1, 256), f32),
            pltpu.VMEM((256, 1152), f32),
            pltpu.VMEM((1, 1152), f32),
            pltpu.VMEM((8, 1, 1152), f32),
            pltpu.VMEM((1, 1152), f32),
            pltpu.VMEM((4, 1, 1152), f32),
            pltpu.SemaphoreType.DMA((10,)),
            pltpu.SemaphoreType.DMA((7,)),
            pltpu.SemaphoreType.DMA((7,)),
            pltpu.SemaphoreType.DMA((3,)),
            pltpu.SemaphoreType.DMA((3,)),
            pltpu.SemaphoreType.DMA,
            pltpu.SemaphoreType.DMA((4, STEPS)),
            pltpu.SemaphoreType.DMA,
        ],
        compiler_params=pltpu.CompilerParams(
            collective_id=0, has_side_effects=True, vmem_limit_bytes=16 * 2**20
        ),
        name="gather",
    )(*(
        pltpu.with_memory_space_constraint(a, pltpu.HBM)
        for a in (
            one_query, other_query, one_key.T, other_key.T, one_value.T, other_value.T,
            mix_share.reshape(1, 256), norm_gain.reshape(1, 256),
        )
    ))
    query, key, value, scale_q, scale_k, scale_v = pl.pallas_call(
        write_kernel,
        out_shape=(
            jax.ShapeDtypeStruct((8192, 1024), bf16),
            jax.ShapeDtypeStruct((64, 8192), bf16),
            jax.ShapeDtypeStruct((64, 8192), bf16),
            jax.ShapeDtypeStruct((1, 1024), f32),
            jax.ShapeDtypeStruct((1, 64), f32),
            jax.ShapeDtypeStruct((1, 64), f32),
        ),
        in_specs=[vmem, vmem],
        out_specs=[hbm] * 4 + [vmem] * 2,
        scratch_shapes=[pltpu.SemaphoreType.DMA((1 + 5 * 32,))],
        compiler_params=pltpu.CompilerParams(vmem_limit_bytes=4 * 2**20),
        name="write",
    )(full, total)
    return (query, key.T, value.T, scale_q.reshape(1024), scale_k.reshape(64), scale_v.reshape(64))


def solution(mesh):
    return jax.shard_map(
        local,
        mesh=mesh,
        in_specs=(
            P("rows", "cols"),
            P("rows", "cols"),
            P("rows", "cols"),
            P("rows", "cols"),
            P("rows", "cols"),
            P("rows", "cols"),
            P("rows"),
            P("rows"),
        ),
        out_specs=(
            P(None, "cols"),
            P(None, "cols"),
            P(None, "cols"),
            P("cols"),
            P("cols"),
            P("cols"),
        ),
        check_vma=False,
    )
```

```python
import functools

import jax
import jax.numpy as jnp
from jax import lax
from jax.experimental import pallas as pl
from jax.experimental.pallas import tpu as pltpu
from jax.sharding import PartitionSpec as P

D_MODEL = 8192
MESH = pl.DeviceIdType.MESH
NX, NY, NC = 4, 4, 2
UNIT = 64

PLUS_X = (
    (0, 0, 0), (0, 0, 1), (0, 0, 2), (-1, 0, 0), (0, 0, 3), (0, -1, 2), (0, 1, 2), (-1, 0, 2),
    (0, 2, 2), (-1, -1, 2), (0, -1, 3), (-1, 1, 2), (0, 1, 3), (-1, 2, 2), (0, 2, 3),
)


def mirrored(items):
    return tuple((-dx, -dy, q ^ 1) for dx, dy, q in items)


def turned(items):
    return tuple((dy, dx, q ^ 2) for dx, dy, q in items)


LINKS = (
    (1, 0, PLUS_X),
    (-1, 0, mirrored(PLUS_X)),
    (0, 1, turned(PLUS_X)),
    (0, -1, mirrored(turned(PLUS_X))),
)


def received(link, slot):
    sx, sy, items = LINKS[link]
    dx, dy, q = items[slot]
    return ((dx - sx) % NX, (dy - sy) % NY, q)


STEPS = len(PLUS_X)
ARRIVAL = {received(link, slot): slot for link in range(4) for slot in range(STEPS)}


def due(link, slot):
    dx, dy, q = LINKS[link][2][slot]
    return -1 if (dx, dy) == (0, 0) else ARRIVAL[(dx % NX, dy % NY, q)]


def gather_kernel(
    one_q, other_q, one_k, other_k, one_v, other_v, mix, gain,
    full, total,
    in_q, in_kv, in_vec,
    gained, part, row_sums, mid, col_sums,
    load_sem, sum_send, sum_recv, send_sem, recv_sem, pair_recv,
):
    me = lax.axis_index("rows")
    core = lax.rem(me, NC)
    chip = lax.div(me, NC)
    x = lax.rem(chip, NX)
    y = lax.div(chip, NX)

    def at(dx, dy):
        return lax.rem(y + dy % NY, NY) * NX + lax.rem(x + dx % NX, NX)

    def device(dx, dy, c):
        return {"rows": at(dx, dy) * NC + c}

    row_peers = [(1, 0, core), (3, 0, core), (2, 0, core), (1, 0, 1 - core), (3, 0, 1 - core), (2, 0, 1 - core), (0, 0, 1 - core)]
    col_peers = [(0, 1, core), (0, 3, core), (0, 2, core)]
    barrier = pltpu.get_barrier_semaphore()
    for peer in row_peers + col_peers:
        pl.semaphore_signal(barrier, inc=1, device_id=device(*peer), device_id_type=MESH)

    small = [
        pltpu.make_async_copy(mix, in_vec.at[0], load_sem.at[0]),
        pltpu.make_async_copy(gain, in_vec.at[1], load_sem.at[0]),
    ]
    thin = [
        pltpu.make_async_copy(one_k, in_kv.at[0, pl.ds(0, 64)], load_sem.at[1]),
        pltpu.make_async_copy(one_v, in_kv.at[0, pl.ds(64, 64)], load_sem.at[1]),
        pltpu.make_async_copy(other_k, in_kv.at[1, pl.ds(0, 64)], load_sem.at[1]),
        pltpu.make_async_copy(other_v, in_kv.at[1, pl.ds(64, 64)], load_sem.at[1]),
    ]
    wide = []
    for h in range(2):
        rows = pl.ds(128 * h, 128)
        wide.append(pltpu.make_async_copy(one_q.at[rows], in_q.at[0, rows], load_sem.at[2 + h]))
        wide.append(pltpu.make_async_copy(other_q.at[rows], in_q.at[1, rows], load_sem.at[2 + h]))
    for copy in small + thin + wide:
        copy.start()
    pltpu.make_async_copy(in_vec, in_vec, load_sem.at[0]).wait()
    pltpu.make_async_copy(in_kv, in_kv, load_sem.at[1]).wait()

    m, g = in_vec[0], in_vec[1]
    kv = (m * in_kv[0] + (1.0 - m) * in_kv[1]) * g
    kv_sum = jnp.sum(jnp.abs(kv), axis=1, keepdims=True)
    gained[pl.ds(0, 128), pl.ds(1024, 128)] = kv[:, :128]
    gained[pl.ds(128, 128), pl.ds(1024, 128)] = kv[:, 128:]
    part[:, pl.ds(1024, 128)] = jnp.transpose(jnp.broadcast_to(kv_sum, (128, 128)))[:1]

    sums = jnp.zeros((8, 1024), jnp.float32)
    for h in range(2):
        half = in_q.at[:, pl.ds(128 * h, 128)]
        pltpu.make_async_copy(half, half, load_sem.at[2 + h]).wait()
        m_rows = jnp.transpose(jnp.broadcast_to(m[:, 128 * h : 128 * h + 128], (128, 128)))
        g_rows = jnp.transpose(jnp.broadcast_to(g[:, 128 * h : 128 * h + 128], (128, 128)))
        for t in range(16):
            rows = pl.ds(128 * h + 8 * t, 8)
            mt = jnp.concatenate([m_rows[8 * t : 8 * t + 8]] * 8, axis=1)
            gt = jnp.concatenate([g_rows[8 * t : 8 * t + 8]] * 8, axis=1)
            value = (mt * in_q[0, rows, :] + (1.0 - mt) * in_q[1, rows, :]) * gt
            gained[rows, pl.ds(0, 1024)] = value
            sums = sums + jnp.abs(value)
    part[:, pl.ds(0, 1024)] = jnp.sum(sums, axis=0, keepdims=True)

    pl.semaphore_wait(barrier, len(row_peers) + len(col_peers))
    own = x * NC + core
    for dx, dy, c in row_peers:
        pltpu.make_async_remote_copy(
            src_ref=part, dst_ref=row_sums.at[own], send_sem=sum_send.at[0],
            recv_sem=sum_recv.at[0], device_id=device(dx, dy, c), device_id_type=MESH,
        ).start()
    row_sums[own] = part[...]
    others = row_sums.at[pl.ds(0, len(row_peers))]
    pltpu.make_async_copy(others, others, sum_recv.at[0]).wait()
    subtotal = row_sums[0]
    for i in range(1, NX * NC):
        subtotal = subtotal + row_sums[i]
    mid[...] = subtotal
    for dx, dy, c in col_peers:
        pltpu.make_async_remote_copy(
            src_ref=mid, dst_ref=col_sums.at[y], send_sem=sum_send.at[1],
            recv_sem=sum_recv.at[1], device_id=device(dx, dy, c), device_id_type=MESH,
        ).start()
    col_sums[y] = mid[...]
    others = col_sums.at[pl.ds(0, len(col_peers))]
    pltpu.make_async_copy(others, others, sum_recv.at[1]).wait()
    subtotal = col_sums[0]
    for i in range(1, NY):
        subtotal = subtotal + col_sums[i]
    scale = subtotal / D_MODEL
    total[...] = scale
    inverse = 1.0 / scale
    inverse_kv = jnp.transpose(jnp.broadcast_to(inverse[:, 1024:], (128, 128)))

    def rows_of(dx, dy, q):
        return pl.ds(pl.multiple_of((core * NX * NY + at(dx, dy)) * 256 + q * UNIT, UNIT), UNIT)

    def send(link, slot):
        sx, sy, items = LINKS[link]
        rows = rows_of(*items[slot])
        pltpu.make_async_remote_copy(
            src_ref=full.at[rows], dst_ref=full.at[rows], send_sem=send_sem,
            recv_sem=recv_sem.at[link, slot], device_id=device(sx, sy, core), device_id_type=MESH,
        ).start()

    def share(dx, dy, q):
        rows = rows_of(dx, dy, q)
        pltpu.make_async_remote_copy(
            src_ref=full.at[rows], dst_ref=full.at[rows], send_sem=send_sem,
            recv_sem=pair_recv, device_id=device(0, 0, 1 - core), device_id_type=MESH,
        ).start()

    for q in range(4):
        rows = pl.ds(q * UNIT, UNIT)
        dst = rows_of(0, 0, q)
        full[dst, pl.ds(0, 1024)] = (gained[rows, pl.ds(0, 1024)] * inverse[:, :1024]).astype(jnp.bfloat16)
        half = (q % 2) * UNIT
        full[dst, pl.ds(1024, 128)] = (gained[rows, pl.ds(1024, 128)] * inverse_kv[half : half + UNIT]).astype(jnp.bfloat16)

    sent = [0, 0, 0, 0]
    for slot in range(-1, STEPS):
        if slot >= 0:
            for link in range(4):
                dx, dy, q = received(link, slot)
                rows = rows_of(dx, dy, q)
                pltpu.make_async_remote_copy(
                    src_ref=full.at[rows], dst_ref=full.at[rows], send_sem=send_sem,
                    recv_sem=recv_sem.at[link, slot], device_id=device(0, 0, 1 - core), device_id_type=MESH,
                ).wait_recv()
                share(dx, dy, q)
        for link in range(4):
            while sent[link] < STEPS and due(link, sent[link]) <= slot:
                send(link, sent[link])
                sent[link] += 1
        if slot == -1:
            for q in range(4):
                share(0, 0, q)

    other = pl.ds(pl.multiple_of((1 - core) * 4096, 4096), 4096)
    pltpu.make_async_copy(full.at[other], full.at[other], pair_recv).wait()
    everything = pl.ds(0, (4 * STEPS + 64) * UNIT)
    pltpu.make_async_copy(full.at[everything], full.at[everything], send_sem).wait()
    sums_sent = row_sums.at[pl.ds(0, len(row_peers))]
    pltpu.make_async_copy(sums_sent, sums_sent, sum_send.at[0]).wait()
    sums_sent = col_sums.at[pl.ds(0, len(col_peers))]
    pltpu.make_async_copy(sums_sent, sums_sent, sum_send.at[1]).wait()


def write_kernel(full, total, query, key, value, scale_q, scale_k, scale_v, near_k, near_v, sem):
    copies = [pltpu.make_async_copy(total.at[:, pl.ds(0, 1024)], scale_q, sem.at[1])]
    for c in range(NC):
        for p in range(NX * NY):
            src, dst = (c * NX * NY + p) * 256, (p * NC + c) * 256
            copies.append(pltpu.make_async_copy(full.at[pl.ds(src, 256), pl.ds(0, 1024)], query.at[pl.ds(dst, 256)], sem.at[0]))
            for q in range(4):
                copies.append(pltpu.make_async_copy(
                    full.at[pl.ds(src + q * UNIT, UNIT), pl.ds(1024, 128)],
                    (key, value)[q % 2].at[:, pl.ds(dst + 128 * (q // 2), 128)],
                    sem.at[0],
                ))
    for copy in copies:
        copy.start()
    near_k[...] = total[:, 1024:1088]
    near_v[...] = total[:, 1088:1152]
    thin = [pltpu.make_async_copy(near_k, scale_k, sem.at[2]), pltpu.make_async_copy(near_v, scale_v, sem.at[3])]
    for copy in thin:
        copy.start()
    for copy in thin:
        copy.wait()
    pltpu.make_async_copy(total.at[:, pl.ds(0, 1024)], scale_q, sem.at[1]).wait()
    pltpu.make_async_copy(full, full, sem.at[0]).wait()


def local(one_query, other_query, one_key, other_key, one_value, other_value, mix_share, norm_gain):
    hbm = pl.BlockSpec(memory_space=pltpu.HBM)
    vmem = pl.BlockSpec(memory_space=pltpu.VMEM)
    f32, bf16 = jnp.float32, jnp.bfloat16
    full, total = pl.pallas_call(
        gather_kernel,
        out_shape=(pltpu.VMEM((8192, 1152), bf16), pltpu.VMEM((1, 1152), f32)),
        in_specs=[hbm] * 8,
        out_specs=(vmem, vmem),
        scratch_shapes=[
            pltpu.VMEM((2, 256, 1024), f32),
            pltpu.VMEM((2, 128, 256), f32),
            pltpu.VMEM((2, 1, 256), f32),
            pltpu.VMEM((256, 1152), f32),
            pltpu.VMEM((1, 1152), f32),
            pltpu.VMEM((8, 1, 1152), f32),
            pltpu.VMEM((1, 1152), f32),
            pltpu.VMEM((4, 1, 1152), f32),
            pltpu.SemaphoreType.DMA((4,)),
            pltpu.SemaphoreType.DMA((2,)),
            pltpu.SemaphoreType.DMA((2,)),
            pltpu.SemaphoreType.DMA,
            pltpu.SemaphoreType.DMA((4, STEPS)),
            pltpu.SemaphoreType.DMA,
        ],
        compiler_params=pltpu.CompilerParams(
            collective_id=0, has_side_effects=True, vmem_limit_bytes=16 * 2**20
        ),
        name="gather",
    )(*(
        pltpu.with_memory_space_constraint(a, pltpu.HBM)
        for a in (
            one_query, other_query, one_key.T, other_key.T, one_value.T, other_value.T,
            mix_share.reshape(1, 256), norm_gain.reshape(1, 256),
        )
    ))
    query, key, value, scale_q, scale_k, scale_v = pl.pallas_call(
        write_kernel,
        out_shape=(
            jax.ShapeDtypeStruct((8192, 1024), bf16),
            jax.ShapeDtypeStruct((64, 8192), bf16),
            jax.ShapeDtypeStruct((64, 8192), bf16),
            jax.ShapeDtypeStruct((1, 1024), f32),
            jax.ShapeDtypeStruct((1, 64), f32),
            jax.ShapeDtypeStruct((1, 64), f32),
        ),
        in_specs=[vmem, vmem],
        out_specs=[hbm] * 6,
        scratch_shapes=[pltpu.VMEM((1, 64), f32), pltpu.VMEM((1, 64), f32), pltpu.SemaphoreType.DMA((4,))],
        compiler_params=pltpu.CompilerParams(vmem_limit_bytes=4 * 2**20),
        name="write",
    )(full, total)
    return (query, key.T, value.T, scale_q.reshape(1024), scale_k.reshape(64), scale_v.reshape(64))


def solution(mesh):
    return jax.shard_map(
        local,
        mesh=mesh,
        in_specs=(
            P("rows", "cols"),
            P("rows", "cols"),
            P("rows", "cols"),
            P("rows", "cols"),
            P("rows", "cols"),
            P("rows", "cols"),
            P("rows"),
            P("rows"),
        ),
        out_specs=(
            P(None, "cols"),
            P(None, "cols"),
            P(None, "cols"),
            P("cols"),
            P("cols"),
            P("cols"),
        ),
        check_vma=False,
    )
```

```python
import functools

import jax
import jax.numpy as jnp
from jax import lax
from jax.experimental import pallas as pl
from jax.experimental.pallas import tpu as pltpu
from jax.sharding import PartitionSpec as P

D_MODEL = 8192
MESH = pl.DeviceIdType.MESH
NX, NY, NC = 4, 4, 2
UNIT = 64

PLUS_X = (
    (0, 0, 0), (0, 0, 1), (0, 0, 2), (-1, 0, 0), (0, 0, 3), (0, -1, 2), (0, 1, 2), (-1, 0, 2),
    (0, 2, 2), (-1, -1, 2), (0, -1, 3), (-1, 1, 2), (0, 1, 3), (-1, 2, 2), (0, 2, 3),
)


def mirrored(items):
    return tuple((-dx, -dy, q ^ 1) for dx, dy, q in items)


def turned(items):
    return tuple((dy, dx, q ^ 2) for dx, dy, q in items)


LINKS = (
    (1, 0, PLUS_X),
    (-1, 0, mirrored(PLUS_X)),
    (0, 1, turned(PLUS_X)),
    (0, -1, mirrored(turned(PLUS_X))),
)


def received(link, slot):
    sx, sy, items = LINKS[link]
    dx, dy, q = items[slot]
    return ((dx - sx) % NX, (dy - sy) % NY, q)


STEPS = len(PLUS_X)
EARLY = ((0, 32), (32, 32))
ARRIVAL = {received(link, slot): slot for link in range(4) for slot in range(STEPS)}


def due(link, slot):
    dx, dy, q = LINKS[link][2][slot]
    return -1 if (dx, dy) == (0, 0) else ARRIVAL[(dx % NX, dy % NY, q)]


def gather_kernel(
    one_q, other_q, one_k, other_k, one_v, other_v, mix, gain,
    full, total,
    in_q, in_kv, in_vec,
    gained, part, row_sums, mid, col_sums, early_in,
    load_sem, sum_send, sum_recv, early_send, early_recv, send_sem, recv_sem, pair_recv,
):
    me = lax.axis_index("rows")
    core = lax.rem(me, NC)
    chip = lax.div(me, NC)
    x = lax.rem(chip, NX)
    y = lax.div(chip, NX)

    def at(dx, dy):
        return lax.rem(y + dy % NY, NY) * NX + lax.rem(x + dx % NX, NX)

    def device(dx, dy, c):
        return {"rows": at(dx, dy) * NC + c}

    row_peers = [(1, 0, core), (3, 0, core), (2, 0, core), (1, 0, 1 - core), (3, 0, 1 - core), (2, 0, 1 - core), (0, 0, 1 - core)]
    col_peers = [(0, 1, core), (0, 3, core), (0, 2, core)]
    barrier = pltpu.get_barrier_semaphore()
    for peer in row_peers + col_peers:
        pl.semaphore_signal(barrier, inc=1, device_id=device(*peer), device_id_type=MESH)

    small = [
        pltpu.make_async_copy(mix, in_vec.at[0], load_sem.at[0]),
        pltpu.make_async_copy(gain, in_vec.at[1], load_sem.at[0]),
    ]
    thin = [
        pltpu.make_async_copy(one_k, in_kv.at[0, pl.ds(0, 64)], load_sem.at[1]),
        pltpu.make_async_copy(one_v, in_kv.at[0, pl.ds(64, 64)], load_sem.at[1]),
        pltpu.make_async_copy(other_k, in_kv.at[1, pl.ds(0, 64)], load_sem.at[1]),
        pltpu.make_async_copy(other_v, in_kv.at[1, pl.ds(64, 64)], load_sem.at[1]),
    ]
    wide = []
    for h in range(2):
        rows = pl.ds(128 * h, 128)
        wide.append(pltpu.make_async_copy(one_q.at[rows], in_q.at[0, rows], load_sem.at[2 + h]))
        wide.append(pltpu.make_async_copy(other_q.at[rows], in_q.at[1, rows], load_sem.at[2 + h]))
    for copy in small + thin + wide:
        copy.start()
    pltpu.make_async_copy(in_vec, in_vec, load_sem.at[0]).wait()
    pltpu.make_async_copy(in_kv, in_kv, load_sem.at[1]).wait()

    m, g = in_vec[0], in_vec[1]
    kv = (m * in_kv[0] + (1.0 - m) * in_kv[1]) * g
    kv_sum = jnp.sum(jnp.abs(kv), axis=1, keepdims=True)
    gained[pl.ds(0, 128), pl.ds(1024, 128)] = kv[:, :128]
    gained[pl.ds(128, 128), pl.ds(1024, 128)] = kv[:, 128:]
    part[:, pl.ds(1024, 128)] = jnp.transpose(jnp.broadcast_to(kv_sum, (128, 128)))[:1]

    sums = jnp.zeros((8, 1024), jnp.float32)
    for h in range(2):
        half = in_q.at[:, pl.ds(128 * h, 128)]
        pltpu.make_async_copy(half, half, load_sem.at[2 + h]).wait()
        m_rows = jnp.transpose(jnp.broadcast_to(m[:, 128 * h : 128 * h + 128], (128, 128)))
        g_rows = jnp.transpose(jnp.broadcast_to(g[:, 128 * h : 128 * h + 128], (128, 128)))
        for t in range(16):
            rows = pl.ds(128 * h + 8 * t, 8)
            mt = jnp.concatenate([m_rows[8 * t : 8 * t + 8]] * 8, axis=1)
            gt = jnp.concatenate([g_rows[8 * t : 8 * t + 8]] * 8, axis=1)
            value = (mt * in_q[0, rows, :] + (1.0 - mt) * in_q[1, rows, :]) * gt
            gained[rows, pl.ds(0, 1024)] = value
            sums = sums + jnp.abs(value)
    part[:, pl.ds(0, 1024)] = jnp.sum(sums, axis=0, keepdims=True)

    pl.semaphore_wait(barrier, len(row_peers) + len(col_peers))
    def early(link, lo, count):
        sx, sy, items = LINKS[link]
        pltpu.make_async_remote_copy(
            src_ref=gained.at[pl.ds(items[0][2] * UNIT + lo, count)], dst_ref=early_in.at[link, pl.ds(lo, count)],
            send_sem=early_send, recv_sem=early_recv, device_id=device(sx, sy, core), device_id_type=MESH,
        ).start()

    own = x * NC + core
    for dx, dy, c in row_peers:
        pltpu.make_async_remote_copy(
            src_ref=part, dst_ref=row_sums.at[own], send_sem=sum_send.at[0],
            recv_sem=sum_recv.at[0], device_id=device(dx, dy, c), device_id_type=MESH,
        ).start()
    for link in (0, 1):
        early(link, 0, UNIT)
    for link in (2, 3):
        early(link, *EARLY[0])
    row_sums[own] = part[...]
    others = row_sums.at[pl.ds(0, len(row_peers))]
    pltpu.make_async_copy(others, others, sum_recv.at[0]).wait()
    subtotal = row_sums[0]
    for i in range(1, NX * NC):
        subtotal = subtotal + row_sums[i]
    mid[...] = subtotal
    for dx, dy, c in col_peers:
        pltpu.make_async_remote_copy(
            src_ref=mid, dst_ref=col_sums.at[y], send_sem=sum_send.at[1],
            recv_sem=sum_recv.at[1], device_id=device(dx, dy, c), device_id_type=MESH,
        ).start()
    for link in (2, 3):
        early(link, *EARLY[1])
    col_sums[y] = mid[...]
    others = col_sums.at[pl.ds(0, len(col_peers))]
    pltpu.make_async_copy(others, others, sum_recv.at[1]).wait()
    subtotal = col_sums[0]
    for i in range(1, NY):
        subtotal = subtotal + col_sums[i]
    scale = subtotal / D_MODEL
    total[...] = scale
    inverse = 1.0 / scale
    inverse_kv = jnp.transpose(jnp.broadcast_to(inverse[:, 1024:], (128, 128)))

    def rows_of(dx, dy, q):
        return pl.ds(pl.multiple_of((core * NX * NY + at(dx, dy)) * 256 + q * UNIT, UNIT), UNIT)

    def send(link, slot):
        sx, sy, items = LINKS[link]
        rows = rows_of(*items[slot])
        pltpu.make_async_remote_copy(
            src_ref=full.at[rows], dst_ref=full.at[rows], send_sem=send_sem,
            recv_sem=recv_sem.at[slot - 1], device_id=device(sx, sy, core), device_id_type=MESH,
        ).start()

    def share(dx, dy, q):
        rows = rows_of(dx, dy, q)
        pltpu.make_async_remote_copy(
            src_ref=full.at[rows], dst_ref=full.at[rows], send_sem=send_sem,
            recv_sem=pair_recv, device_id=device(0, 0, 1 - core), device_id_type=MESH,
        ).start()

    def finish(dst, q, value):
        half = (q % 2) * UNIT
        full[dst, pl.ds(0, 1024)] = (value[:, :1024] * inverse[:, :1024]).astype(jnp.bfloat16)
        full[dst, pl.ds(1024, 128)] = (value[:, 1024:] * inverse_kv[half : half + UNIT]).astype(jnp.bfloat16)

    for q in range(4):
        finish(rows_of(0, 0, q), q, gained[pl.ds(q * UNIT, UNIT), :])

    sent = [1, 1, 1, 1]
    for slot in range(-1, STEPS):
        if slot == 0:
            pltpu.make_async_copy(early_in, early_in, early_recv).wait()
        elif slot > 0:
            four = pl.ds(0, 4 * UNIT)
            pltpu.make_async_copy(full.at[four], full.at[four], recv_sem.at[slot - 1]).wait()
        for link in range(4 if slot >= 0 else 0):
            dx, dy, q = received(link, slot)
            if slot == 0:
                finish(rows_of(dx, dy, q), q, early_in[link])
            share(dx, dy, q)
        for link in range(4):
            while sent[link] < STEPS and due(link, sent[link]) <= slot:
                send(link, sent[link])
                sent[link] += 1
        if slot == -1:
            for q in range(4):
                share(0, 0, q)

    other = pl.ds(pl.multiple_of((1 - core) * 4096, 4096), 4096)
    pltpu.make_async_copy(full.at[other], full.at[other], pair_recv).wait()
    everything = pl.ds(0, (4 * (STEPS - 1) + 64) * UNIT)
    pltpu.make_async_copy(full.at[everything], full.at[everything], send_sem).wait()
    pltpu.make_async_copy(gained, gained, early_send).wait()
    sums_sent = row_sums.at[pl.ds(0, len(row_peers))]
    pltpu.make_async_copy(sums_sent, sums_sent, sum_send.at[0]).wait()
    sums_sent = col_sums.at[pl.ds(0, len(col_peers))]
    pltpu.make_async_copy(sums_sent, sums_sent, sum_send.at[1]).wait()


def write_kernel(full, total, query, key, value, scale_q, scale_k, scale_v, near_k, near_v, sem):
    copies = [pltpu.make_async_copy(total.at[:, pl.ds(0, 1024)], scale_q, sem.at[1])]
    for c in range(NC):
        for p in range(NX * NY):
            src, dst = (c * NX * NY + p) * 256, (p * NC + c) * 256
            copies.append(pltpu.make_async_copy(full.at[pl.ds(src, 256), pl.ds(0, 1024)], query.at[pl.ds(dst, 256)], sem.at[0]))
            for q in range(4):
                copies.append(pltpu.make_async_copy(
                    full.at[pl.ds(src + q * UNIT, UNIT), pl.ds(1024, 128)],
                    (key, value)[q % 2].at[:, pl.ds(dst + 128 * (q // 2), 128)],
                    sem.at[0],
                ))
    for copy in copies:
        copy.start()
    near_k[...] = total[:, 1024:1088]
    near_v[...] = total[:, 1088:1152]
    thin = [pltpu.make_async_copy(near_k, scale_k, sem.at[2]), pltpu.make_async_copy(near_v, scale_v, sem.at[3])]
    for copy in thin:
        copy.start()
    for copy in thin:
        copy.wait()
    pltpu.make_async_copy(total.at[:, pl.ds(0, 1024)], scale_q, sem.at[1]).wait()
    pltpu.make_async_copy(full, full, sem.at[0]).wait()


def local(one_query, other_query, one_key, other_key, one_value, other_value, mix_share, norm_gain):
    hbm = pl.BlockSpec(memory_space=pltpu.HBM)
    vmem = pl.BlockSpec(memory_space=pltpu.VMEM)
    f32, bf16 = jnp.float32, jnp.bfloat16
    full, total = pl.pallas_call(
        gather_kernel,
        out_shape=(pltpu.VMEM((8192, 1152), bf16), pltpu.VMEM((1, 1152), f32)),
        in_specs=[hbm] * 8,
        out_specs=(vmem, vmem),
        scratch_shapes=[
            pltpu.VMEM((2, 256, 1024), f32),
            pltpu.VMEM((2, 128, 256), f32),
            pltpu.VMEM((2, 1, 256), f32),
            pltpu.VMEM((256, 1152), f32),
            pltpu.VMEM((1, 1152), f32),
            pltpu.VMEM((8, 1, 1152), f32),
            pltpu.VMEM((1, 1152), f32),
            pltpu.VMEM((4, 1, 1152), f32),
            pltpu.VMEM((4, UNIT, 1152), f32),
            pltpu.SemaphoreType.DMA((4,)),
            pltpu.SemaphoreType.DMA((2,)),
            pltpu.SemaphoreType.DMA((2,)),
            pltpu.SemaphoreType.DMA,
            pltpu.SemaphoreType.DMA,
            pltpu.SemaphoreType.DMA,
            pltpu.SemaphoreType.DMA((STEPS - 1,)),
            pltpu.SemaphoreType.DMA,
        ],
        compiler_params=pltpu.CompilerParams(
            collective_id=0, has_side_effects=True, vmem_limit_bytes=16 * 2**20
        ),
        name="gather",
    )(*(
        pltpu.with_memory_space_constraint(a, pltpu.HBM)
        for a in (
            one_query, other_query, one_key.T, other_key.T, one_value.T, other_value.T,
            mix_share.reshape(1, 256), norm_gain.reshape(1, 256),
        )
    ))
    query, key, value, scale_q, scale_k, scale_v = pl.pallas_call(
        write_kernel,
        out_shape=(
            jax.ShapeDtypeStruct((8192, 1024), bf16),
            jax.ShapeDtypeStruct((64, 8192), bf16),
            jax.ShapeDtypeStruct((64, 8192), bf16),
            jax.ShapeDtypeStruct((1, 1024), f32),
            jax.ShapeDtypeStruct((1, 64), f32),
            jax.ShapeDtypeStruct((1, 64), f32),
        ),
        in_specs=[vmem, vmem],
        out_specs=[hbm] * 6,
        scratch_shapes=[pltpu.VMEM((1, 64), f32), pltpu.VMEM((1, 64), f32), pltpu.SemaphoreType.DMA((4,))],
        compiler_params=pltpu.CompilerParams(vmem_limit_bytes=4 * 2**20),
        name="write",
    )(full, total)
    return (query, key.T, value.T, scale_q.reshape(1024), scale_k.reshape(64), scale_v.reshape(64))


def solution(mesh):
    return jax.shard_map(
        local,
        mesh=mesh,
        in_specs=(
            P("rows", "cols"),
            P("rows", "cols"),
            P("rows", "cols"),
            P("rows", "cols"),
            P("rows", "cols"),
            P("rows", "cols"),
            P("rows"),
            P("rows"),
        ),
        out_specs=(
            P(None, "cols"),
            P(None, "cols"),
            P(None, "cols"),
            P("cols"),
            P("cols"),
            P("cols"),
        ),
        check_vma=False,
    )
```

```python
import functools

import jax
import jax.numpy as jnp
from jax import lax
from jax.experimental import pallas as pl
from jax.experimental.pallas import tpu as pltpu
from jax.sharding import PartitionSpec as P

D_MODEL = 8192
MESH = pl.DeviceIdType.MESH
NX, NY, NC = 4, 4, 2
UNIT = 64

PLUS_X = (
    (0, 0, 0), (0, 0, 1), (0, 0, 2), (-1, 0, 0), (0, 0, 3), (0, -1, 2), (0, 1, 2), (-1, 0, 2),
    (0, 2, 2), (-1, -1, 2), (0, -1, 3), (-1, 1, 2), (0, 1, 3), (-1, 2, 2), (0, 2, 3),
)


def mirrored(items):
    return tuple((-dx, -dy, q ^ 1) for dx, dy, q in items)


def turned(items):
    return tuple((dy, dx, q ^ 2) for dx, dy, q in items)


LINKS = (
    (1, 0, PLUS_X),
    (-1, 0, mirrored(PLUS_X)),
    (0, 1, turned(PLUS_X)),
    (0, -1, mirrored(turned(PLUS_X))),
)


def received(link, slot):
    sx, sy, items = LINKS[link]
    dx, dy, q = items[slot]
    return ((dx - sx) % NX, (dy - sy) % NY, q)


STEPS = len(PLUS_X)
PIECES = [((0, UNIT),)] * (STEPS - 1) + [((0, 32), (32, 16), (48, 16))]
FLAG = [sum(len(p) for p in PIECES[1:slot]) for slot in range(STEPS + 1)]
EARLY = ((0, 32), (32, 32))
ARRIVAL = {received(link, slot): slot for link in range(4) for slot in range(STEPS)}


def due(link, slot):
    dx, dy, q = LINKS[link][2][slot]
    return -1 if (dx, dy) == (0, 0) else ARRIVAL[(dx % NX, dy % NY, q)]


def gather_kernel(
    one_q, other_q, one_k, other_k, one_v, other_v, mix, gain,
    full, total,
    in_q, in_kv, in_vec,
    gained, part, row_sums, mid, col_sums, early_in,
    load_sem, sum_send, sum_recv, early_send, early_recv, send_sem, recv_sem, pair_recv,
):
    me = lax.axis_index("rows")
    core = lax.rem(me, NC)
    chip = lax.div(me, NC)
    x = lax.rem(chip, NX)
    y = lax.div(chip, NX)

    def at(dx, dy):
        return lax.rem(y + dy % NY, NY) * NX + lax.rem(x + dx % NX, NX)

    def device(dx, dy, c):
        return {"rows": at(dx, dy) * NC + c}

    row_peers = [(2, 0, core), (2, 0, 1 - core), (1, 0, core), (3, 0, core), (1, 0, 1 - core), (3, 0, 1 - core), (0, 0, 1 - core)]
    col_peers = [(0, 2, core), (0, 1, core), (0, 3, core)]
    small = [
        pltpu.make_async_copy(mix, in_vec.at[0], load_sem.at[0]),
        pltpu.make_async_copy(gain, in_vec.at[1], load_sem.at[0]),
    ]
    thin = [
        pltpu.make_async_copy(one_k, in_kv.at[0, pl.ds(0, 64)], load_sem.at[1]),
        pltpu.make_async_copy(one_v, in_kv.at[0, pl.ds(64, 64)], load_sem.at[1]),
        pltpu.make_async_copy(other_k, in_kv.at[1, pl.ds(0, 64)], load_sem.at[1]),
        pltpu.make_async_copy(other_v, in_kv.at[1, pl.ds(64, 64)], load_sem.at[1]),
    ]
    wide = []
    for h in range(2):
        rows = pl.ds(128 * h, 128)
        wide.append(pltpu.make_async_copy(one_q.at[rows], in_q.at[0, rows], load_sem.at[2 + h]))
        wide.append(pltpu.make_async_copy(other_q.at[rows], in_q.at[1, rows], load_sem.at[2 + h]))
    for copy in small + thin + wide:
        copy.start()
    barrier = pltpu.get_barrier_semaphore()
    for peer in row_peers + col_peers:
        pl.semaphore_signal(barrier, inc=1, device_id=device(*peer), device_id_type=MESH)
    pltpu.make_async_copy(in_vec, in_vec, load_sem.at[0]).wait()
    pltpu.make_async_copy(in_kv, in_kv, load_sem.at[1]).wait()

    m, g = in_vec[0], in_vec[1]
    kv = (m * in_kv[0] + (1.0 - m) * in_kv[1]) * g
    kv_sum = jnp.sum(jnp.abs(kv), axis=1, keepdims=True)
    gained[pl.ds(0, 128), pl.ds(1024, 128)] = kv[:, :128]
    gained[pl.ds(128, 128), pl.ds(1024, 128)] = kv[:, 128:]
    part[:, pl.ds(1024, 128)] = jnp.transpose(jnp.broadcast_to(kv_sum, (128, 128)))[:1]

    sums = jnp.zeros((8, 1024), jnp.float32)
    for h in range(2):
        half = in_q.at[:, pl.ds(128 * h, 128)]
        pltpu.make_async_copy(half, half, load_sem.at[2 + h]).wait()
        m_rows = jnp.transpose(jnp.broadcast_to(m[:, 128 * h : 128 * h + 128], (128, 128)))
        g_rows = jnp.transpose(jnp.broadcast_to(g[:, 128 * h : 128 * h + 128], (128, 128)))
        for t in range(16):
            rows = pl.ds(128 * h + 8 * t, 8)
            mt = jnp.concatenate([m_rows[8 * t : 8 * t + 8]] * 8, axis=1)
            gt = jnp.concatenate([g_rows[8 * t : 8 * t + 8]] * 8, axis=1)
            value = (mt * in_q[0, rows, :] + (1.0 - mt) * in_q[1, rows, :]) * gt
            gained[rows, pl.ds(0, 1024)] = value
            sums = sums + jnp.abs(value)
    part[:, pl.ds(0, 1024)] = jnp.sum(sums, axis=0, keepdims=True)

    pl.semaphore_wait(barrier, len(row_peers) + len(col_peers))
    def early(link, lo, count):
        sx, sy, items = LINKS[link]
        pltpu.make_async_remote_copy(
            src_ref=gained.at[pl.ds(items[0][2] * UNIT + lo, count)], dst_ref=early_in.at[link, pl.ds(lo, count)],
            send_sem=early_send, recv_sem=early_recv, device_id=device(sx, sy, core), device_id_type=MESH,
        ).start()

    own = x * NC + core
    for dx, dy, c in row_peers:
        pltpu.make_async_remote_copy(
            src_ref=part, dst_ref=row_sums.at[own], send_sem=sum_send.at[0],
            recv_sem=sum_recv.at[0], device_id=device(dx, dy, c), device_id_type=MESH,
        ).start()
    for link in (0, 1):
        early(link, 0, UNIT)
    for link in (2, 3):
        early(link, *EARLY[0])
    row_sums[own] = part[...]
    others = row_sums.at[pl.ds(0, len(row_peers))]
    pltpu.make_async_copy(others, others, sum_recv.at[0]).wait()
    subtotal = row_sums[0]
    for i in range(1, NX * NC):
        subtotal = subtotal + row_sums[i]
    mid[...] = subtotal
    for dx, dy, c in col_peers:
        pltpu.make_async_remote_copy(
            src_ref=mid, dst_ref=col_sums.at[y], send_sem=sum_send.at[1],
            recv_sem=sum_recv.at[1], device_id=device(dx, dy, c), device_id_type=MESH,
        ).start()
    for link in (2, 3):
        early(link, *EARLY[1])
    col_sums[y] = mid[...]
    others = col_sums.at[pl.ds(0, len(col_peers))]
    pltpu.make_async_copy(others, others, sum_recv.at[1]).wait()
    subtotal = col_sums[0]
    for i in range(1, NY):
        subtotal = subtotal + col_sums[i]
    scale = subtotal / D_MODEL
    total[...] = scale
    inverse = 1.0 / scale
    inverse_kv = jnp.transpose(jnp.broadcast_to(inverse[:, 1024:], (128, 128)))

    def rows_of(dx, dy, q, lo=0, count=UNIT):
        return pl.ds(pl.multiple_of((core * NX * NY + at(dx, dy)) * 256 + q * UNIT + lo, 16), count)

    def send(link, slot):
        sx, sy, items = LINKS[link]
        for piece, (lo, count) in enumerate(PIECES[slot]):
            rows = rows_of(*items[slot], lo, count)
            pltpu.make_async_remote_copy(
                src_ref=full.at[rows], dst_ref=full.at[rows], send_sem=send_sem,
                recv_sem=recv_sem.at[FLAG[slot] + piece], device_id=device(sx, sy, core), device_id_type=MESH,
            ).start()

    def share(dx, dy, q, lo=0, count=UNIT):
        rows = rows_of(dx, dy, q, lo, count)
        pltpu.make_async_remote_copy(
            src_ref=full.at[rows], dst_ref=full.at[rows], send_sem=send_sem,
            recv_sem=pair_recv, device_id=device(0, 0, 1 - core), device_id_type=MESH,
        ).start()

    def finish(dst, q, value):
        half = (q % 2) * UNIT
        full[dst, pl.ds(0, 1024)] = (value[:, :1024] * inverse[:, :1024]).astype(jnp.bfloat16)
        full[dst, pl.ds(1024, 128)] = (value[:, 1024:] * inverse_kv[half : half + UNIT]).astype(jnp.bfloat16)

    for q in range(4):
        finish(rows_of(0, 0, q), q, gained[pl.ds(q * UNIT, UNIT), :])

    sent = [1, 1, 1, 1]
    for slot in range(-1, STEPS):
        if slot == 0:
            pltpu.make_async_copy(early_in, early_in, early_recv).wait()
            for link in range(4):
                dx, dy, q = received(link, slot)
                finish(rows_of(dx, dy, q), q, early_in[link])
                share(dx, dy, q)
        elif slot > 0:
            for piece, (lo, count) in enumerate(PIECES[slot]):
                four = pl.ds(0, 4 * count)
                pltpu.make_async_copy(full.at[four], full.at[four], recv_sem.at[FLAG[slot] + piece]).wait()
                for link in range(4):
                    share(*received(link, slot), lo, count)
        for link in range(4):
            while sent[link] < STEPS and due(link, sent[link]) <= slot:
                send(link, sent[link])
                sent[link] += 1
        if slot == -1:
            for q in range(4):
                share(0, 0, q)

    other = pl.ds(pl.multiple_of((1 - core) * 4096, 4096), 4096)
    pltpu.make_async_copy(full.at[other], full.at[other], pair_recv).wait()
    everything = pl.ds(0, (4 * (STEPS - 1) + 64) * UNIT)
    pltpu.make_async_copy(full.at[everything], full.at[everything], send_sem).wait()
    pltpu.make_async_copy(gained, gained, early_send).wait()
    sums_sent = row_sums.at[pl.ds(0, len(row_peers))]
    pltpu.make_async_copy(sums_sent, sums_sent, sum_send.at[0]).wait()
    sums_sent = col_sums.at[pl.ds(0, len(col_peers))]
    pltpu.make_async_copy(sums_sent, sums_sent, sum_send.at[1]).wait()


def write_kernel(full, total, query, key, value, scale_q, scale_k, scale_v, near_k, near_v, sem):
    copies = [pltpu.make_async_copy(total.at[:, pl.ds(0, 1024)], scale_q, sem.at[1])]
    for c in range(NC):
        for p in range(NX * NY):
            src, dst = (c * NX * NY + p) * 256, (p * NC + c) * 256
            copies.append(pltpu.make_async_copy(full.at[pl.ds(src, 256), pl.ds(0, 1024)], query.at[pl.ds(dst, 256)], sem.at[0]))
            for q in range(4):
                copies.append(pltpu.make_async_copy(
                    full.at[pl.ds(src + q * UNIT, UNIT), pl.ds(1024, 128)],
                    (key, value)[q % 2].at[:, pl.ds(dst + 128 * (q // 2), 128)],
                    sem.at[0],
                ))
    for copy in copies:
        copy.start()
    near_k[...] = total[:, 1024:1088]
    near_v[...] = total[:, 1088:1152]
    thin = [pltpu.make_async_copy(near_k, scale_k, sem.at[2]), pltpu.make_async_copy(near_v, scale_v, sem.at[3])]
    for copy in thin:
        copy.start()
    for copy in thin:
        copy.wait()
    pltpu.make_async_copy(total.at[:, pl.ds(0, 1024)], scale_q, sem.at[1]).wait()
    pltpu.make_async_copy(full, full, sem.at[0]).wait()


def local(one_query, other_query, one_key, other_key, one_value, other_value, mix_share, norm_gain):
    hbm = pl.BlockSpec(memory_space=pltpu.HBM)
    vmem = pl.BlockSpec(memory_space=pltpu.VMEM)
    f32, bf16 = jnp.float32, jnp.bfloat16
    full, total = pl.pallas_call(
        gather_kernel,
        out_shape=(pltpu.VMEM((8192, 1152), bf16), pltpu.VMEM((1, 1152), f32)),
        in_specs=[hbm] * 8,
        out_specs=(vmem, vmem),
        scratch_shapes=[
            pltpu.VMEM((2, 256, 1024), f32),
            pltpu.VMEM((2, 128, 256), f32),
            pltpu.VMEM((2, 1, 256), f32),
            pltpu.VMEM((256, 1152), f32),
            pltpu.VMEM((1, 1152), f32),
            pltpu.VMEM((8, 1, 1152), f32),
            pltpu.VMEM((1, 1152), f32),
            pltpu.VMEM((4, 1, 1152), f32),
            pltpu.VMEM((4, UNIT, 1152), f32),
            pltpu.SemaphoreType.DMA((4,)),
            pltpu.SemaphoreType.DMA((2,)),
            pltpu.SemaphoreType.DMA((2,)),
            pltpu.SemaphoreType.DMA,
            pltpu.SemaphoreType.DMA,
            pltpu.SemaphoreType.DMA,
            pltpu.SemaphoreType.DMA((FLAG[STEPS],)),
            pltpu.SemaphoreType.DMA,
        ],
        compiler_params=pltpu.CompilerParams(
            collective_id=0, has_side_effects=True, vmem_limit_bytes=16 * 2**20
        ),
        name="gather",
    )(*(
        pltpu.with_memory_space_constraint(a, pltpu.HBM)
        for a in (
            one_query, other_query, one_key.T, other_key.T, one_value.T, other_value.T,
            mix_share.reshape(1, 256), norm_gain.reshape(1, 256),
        )
    ))
    query, key, value, scale_q, scale_k, scale_v = pl.pallas_call(
        write_kernel,
        out_shape=(
            jax.ShapeDtypeStruct((8192, 1024), bf16),
            jax.ShapeDtypeStruct((64, 8192), bf16),
            jax.ShapeDtypeStruct((64, 8192), bf16),
            jax.ShapeDtypeStruct((1, 1024), f32),
            jax.ShapeDtypeStruct((1, 64), f32),
            jax.ShapeDtypeStruct((1, 64), f32),
        ),
        in_specs=[vmem, vmem],
        out_specs=[hbm] * 6,
        scratch_shapes=[pltpu.VMEM((1, 64), f32), pltpu.VMEM((1, 64), f32), pltpu.SemaphoreType.DMA((4,))],
        compiler_params=pltpu.CompilerParams(vmem_limit_bytes=4 * 2**20),
        name="write",
    )(full, total)
    return (query, key.T, value.T, scale_q.reshape(1024), scale_k.reshape(64), scale_v.reshape(64))


def solution(mesh):
    return jax.shard_map(
        local,
        mesh=mesh,
        in_specs=(
            P("rows", "cols"),
            P("rows", "cols"),
            P("rows", "cols"),
            P("rows", "cols"),
            P("rows", "cols"),
            P("rows", "cols"),
            P("rows"),
            P("rows"),
        ),
        out_specs=(
            P(None, "cols"),
            P(None, "cols"),
            P(None, "cols"),
            P("cols"),
            P("cols"),
            P("cols"),
        ),
        check_vma=False,
    )
```

```python
import functools

import jax
import jax.numpy as jnp
from jax import lax
from jax.experimental import pallas as pl
from jax.experimental.pallas import tpu as pltpu
from jax.sharding import PartitionSpec as P

D_MODEL = 8192
MESH = pl.DeviceIdType.MESH
NX, NY, NC = 4, 4, 2
UNIT = 64

PLUS_X = (
    (0, 0, 0), (0, 0, 1), (0, 0, 2), (-1, 0, 0), (0, 0, 3), (0, -1, 2), (0, 1, 2), (-1, 0, 2),
    (0, 2, 2), (-1, -1, 2), (0, -1, 3), (-1, 1, 2), (0, 1, 3), (-1, 2, 2), (0, 2, 3),
)


def mirrored(items):
    return tuple((-dx, -dy, q ^ 1) for dx, dy, q in items)


def turned(items):
    return tuple((dy, dx, q ^ 2) for dx, dy, q in items)


LINKS = (
    (1, 0, PLUS_X),
    (-1, 0, mirrored(PLUS_X)),
    (0, 1, turned(PLUS_X)),
    (0, -1, mirrored(turned(PLUS_X))),
)


def received(link, slot):
    sx, sy, items = LINKS[link]
    dx, dy, q = items[slot]
    return ((dx - sx) % NX, (dy - sy) % NY, q)


STEPS = len(PLUS_X)
PIECES = [((0, UNIT),)] * (STEPS - 1) + [((0, 32), (32, 16), (48, 16))]
FLAG = [sum(len(p) for p in PIECES[1:slot]) for slot in range(STEPS + 1)]
SPLIT = (12, 6)
READY = 10
PACE = 10
FIRST = SPLIT.index(min(SPLIT))
EARLY = ((0, 32), (32, 32))
ARRIVAL = {received(link, slot): slot for link in range(4) for slot in range(STEPS)}


def due(link, slot):
    dx, dy, q = LINKS[link][2][slot]
    return -1 if (dx, dy) == (0, 0) else ARRIVAL[(dx % NX, dy % NY, q)]


def gather_kernel(
    one_q, other_q, one_k, other_k, one_v, other_v, mix, gain,
    full, total,
    in_q, in_kv, in_vec,
    gained, part, row_sums, mid, col_sums, early_in,
    load_sem, sum_send, sum_recv, early_send, early_recv, send_sem, recv_sem, pair_recv,
):
    me = lax.axis_index("rows")
    core = lax.rem(me, NC)
    chip = lax.div(me, NC)
    x = lax.rem(chip, NX)
    y = lax.div(chip, NX)

    def at(dx, dy):
        return lax.rem(y + dy % NY, NY) * NX + lax.rem(x + dx % NX, NX)

    def device(dx, dy, c):
        return {"rows": at(dx, dy) * NC + c}

    row_peers = [(2, 0, core), (2, 0, 1 - core), (1, 0, core), (3, 0, core), (1, 0, 1 - core), (3, 0, 1 - core), (0, 0, 1 - core)]
    col_peers = [(0, 2, core), (0, 1, core), (0, 3, core)]
    small = [
        pltpu.make_async_copy(mix, in_vec.at[0], load_sem.at[0]),
        pltpu.make_async_copy(gain, in_vec.at[1], load_sem.at[0]),
    ]
    thin = [
        pltpu.make_async_copy(one_k, in_kv.at[0, pl.ds(0, 64)], load_sem.at[1]),
        pltpu.make_async_copy(one_v, in_kv.at[0, pl.ds(64, 64)], load_sem.at[1]),
        pltpu.make_async_copy(other_k, in_kv.at[1, pl.ds(0, 64)], load_sem.at[1]),
        pltpu.make_async_copy(other_v, in_kv.at[1, pl.ds(64, 64)], load_sem.at[1]),
    ]
    wide = []
    for h in range(2):
        rows = pl.ds(128 * h, 128)
        wide.append(pltpu.make_async_copy(one_q.at[rows], in_q.at[0, rows], load_sem.at[2 + h]))
        wide.append(pltpu.make_async_copy(other_q.at[rows], in_q.at[1, rows], load_sem.at[2 + h]))
    for copy in small + thin + wide:
        copy.start()
    barrier = pltpu.get_barrier_semaphore()
    for peer in row_peers + col_peers:
        pl.semaphore_signal(barrier, inc=1, device_id=device(*peer), device_id_type=MESH)
    pltpu.make_async_copy(in_vec, in_vec, load_sem.at[0]).wait()
    pltpu.make_async_copy(in_kv, in_kv, load_sem.at[1]).wait()

    m, g = in_vec[0], in_vec[1]
    kv = (m * in_kv[0] + (1.0 - m) * in_kv[1]) * g
    kv_sum = jnp.sum(jnp.abs(kv), axis=1, keepdims=True)
    gained[pl.ds(0, 128), pl.ds(1024, 128)] = kv[:, :128]
    gained[pl.ds(128, 128), pl.ds(1024, 128)] = kv[:, 128:]
    part[:, pl.ds(1024, 128)] = jnp.transpose(jnp.broadcast_to(kv_sum, (128, 128)))[:1]

    sums = jnp.zeros((8, 1024), jnp.float32)
    for h in range(2):
        half = in_q.at[:, pl.ds(128 * h, 128)]
        pltpu.make_async_copy(half, half, load_sem.at[2 + h]).wait()
        m_rows = jnp.transpose(jnp.broadcast_to(m[:, 128 * h : 128 * h + 128], (128, 128)))
        g_rows = jnp.transpose(jnp.broadcast_to(g[:, 128 * h : 128 * h + 128], (128, 128)))
        for t in range(16):
            rows = pl.ds(128 * h + 8 * t, 8)
            mt = jnp.concatenate([m_rows[8 * t : 8 * t + 8]] * 8, axis=1)
            gt = jnp.concatenate([g_rows[8 * t : 8 * t + 8]] * 8, axis=1)
            value = (mt * in_q[0, rows, :] + (1.0 - mt) * in_q[1, rows, :]) * gt
            gained[rows, pl.ds(0, 1024)] = value
            sums = sums + jnp.abs(value)
    part[:, pl.ds(0, 1024)] = jnp.sum(sums, axis=0, keepdims=True)

    pl.semaphore_wait(barrier, len(row_peers) + len(col_peers))
    def early(link, lo, count):
        sx, sy, items = LINKS[link]
        pltpu.make_async_remote_copy(
            src_ref=gained.at[pl.ds(items[0][2] * UNIT + lo, count)], dst_ref=early_in.at[link, pl.ds(lo, count)],
            send_sem=early_send, recv_sem=early_recv, device_id=device(sx, sy, core), device_id_type=MESH,
        ).start()

    own = x * NC + core
    for dx, dy, c in row_peers:
        pltpu.make_async_remote_copy(
            src_ref=part, dst_ref=row_sums.at[own], send_sem=sum_send.at[0],
            recv_sem=sum_recv.at[0], device_id=device(dx, dy, c), device_id_type=MESH,
        ).start()
    for link in (0, 1):
        early(link, 0, UNIT)
    for link in (2, 3):
        early(link, *EARLY[0])
    row_sums[own] = part[...]
    others = row_sums.at[pl.ds(0, len(row_peers))]
    pltpu.make_async_copy(others, others, sum_recv.at[0]).wait()
    subtotal = row_sums[0]
    for i in range(1, NX * NC):
        subtotal = subtotal + row_sums[i]
    mid[...] = subtotal
    for dx, dy, c in col_peers:
        pltpu.make_async_remote_copy(
            src_ref=mid, dst_ref=col_sums.at[y], send_sem=sum_send.at[1],
            recv_sem=sum_recv.at[1], device_id=device(dx, dy, c), device_id_type=MESH,
        ).start()
    for link in (2, 3):
        early(link, *EARLY[1])
    col_sums[y] = mid[...]
    others = col_sums.at[pl.ds(0, len(col_peers))]
    pltpu.make_async_copy(others, others, sum_recv.at[1]).wait()
    subtotal = col_sums[0]
    for i in range(1, NY):
        subtotal = subtotal + col_sums[i]
    scale = subtotal / D_MODEL
    total[...] = scale
    inverse = 1.0 / scale
    inverse_kv = jnp.transpose(jnp.broadcast_to(inverse[:, 1024:], (128, 128)))

    def rows_of(dx, dy, q):
        return pl.ds(pl.multiple_of((core * NX * NY + at(dx, dy)) * 256 + q * UNIT, UNIT), UNIT)

    def send(link, slot):
        sx, sy, items = LINKS[link]
        rows = rows_of(*items[slot])
        pltpu.make_async_remote_copy(
            src_ref=full.at[rows], dst_ref=full.at[rows], send_sem=send_sem,
            recv_sem=recv_sem.at[slot], device_id=device(sx, sy, core), device_id_type=MESH,
        ).start()

    def share(dx, dy, q):
        rows = rows_of(dx, dy, q)
        pltpu.make_async_remote_copy(
            src_ref=full.at[rows], dst_ref=full.at[rows], send_sem=send_sem,
            recv_sem=pair_recv, device_id=device(0, 0, 1 - core), device_id_type=MESH,
        ).start()

    def finish(dst, q, value):
        half = (q % 2) * UNIT
        full[dst, pl.ds(0, 1024)] = (value[:, :1024] * inverse[:, :1024]).astype(jnp.bfloat16)
        full[dst, pl.ds(1024, 128)] = (value[:, 1024:] * inverse_kv[half : half + UNIT]).astype(jnp.bfloat16)

    for q in range(4):
        finish(rows_of(0, 0, q), q, gained[pl.ds(q * UNIT, UNIT), :])

    def run(c):
        sent = [1, 1, 1, 1]
        for slot in range(-1, SPLIT[c]):
            if slot == 0:
                pltpu.make_async_copy(early_in, early_in, early_recv).wait()
                for link in range(4):
                    dx, dy, q = received(link, slot)
                    finish(rows_of(dx, dy, q), q, early_in[link])
                    share(dx, dy, q)
            elif slot > 0:
                four = pl.ds(0, 4 * UNIT)
                pltpu.make_async_copy(full.at[four], full.at[four], recv_sem.at[slot]).wait()
                if slot < min(SPLIT):
                    for link in range(4):
                        share(*received(link, slot))
            for link in range(4):
                while sent[link] < SPLIT[c] and due(link, sent[link]) <= slot:
                    send(link, sent[link])
                    sent[link] += 1
            if slot == -1:
                for q in range(4):
                    share(0, 0, q)
        other = pl.ds(0, (4 + 4 * min(SPLIT)) * UNIT)
        pltpu.make_async_copy(full.at[other], full.at[other], pair_recv).wait()
        everything = pl.ds(0, (4 * (SPLIT[c] - 1) + 4 + 4 * min(SPLIT)) * UNIT)
        pltpu.make_async_copy(full.at[everything], full.at[everything], send_sem).wait()

    for c in range(NC):
        pl.when(core == c)(functools.partial(run, c))
    pltpu.make_async_copy(gained, gained, early_send).wait()
    sums_sent = row_sums.at[pl.ds(0, len(row_peers))]
    pltpu.make_async_copy(sums_sent, sums_sent, sum_send.at[0]).wait()
    sums_sent = col_sums.at[pl.ds(0, len(col_peers))]
    pltpu.make_async_copy(sums_sent, sums_sent, sum_send.at[1]).wait()


def rest_kernel(first, token, full, send_sem, recv_sem, pair_recv, ready):
    me = lax.axis_index("rows")
    core = lax.rem(me, NC)
    chip = lax.div(me, NC)
    x = lax.rem(chip, NX)
    y = lax.div(chip, NX)

    def at(dx, dy):
        return lax.rem(y + dy % NY, NY) * NX + lax.rem(x + dx % NX, NX)

    def device(dx, dy, c):
        return {"rows": at(dx, dy) * NC + c}

    barrier = pltpu.get_barrier_semaphore()
    for sx, sy, _ in LINKS:
        pl.semaphore_signal(barrier, inc=1, device_id=device(sx, sy, core), device_id_type=MESH)

    def run(c):
        if c == FIRST:
            pl.semaphore_signal(barrier, inc=1, device_id=device(0, 0, 1 - FIRST), device_id_type=MESH)
        pl.semaphore_wait(barrier, 4 if c == FIRST else 5)
        if c != FIRST:
            pl.semaphore_signal(ready, inc=1, device_id=device(0, 0, FIRST), device_id_type=MESH)

        def rows_of(dx, dy, q, lo=0, count=UNIT):
            return pl.ds(pl.multiple_of((c * NX * NY + at(dx, dy)) * 256 + q * UNIT + lo, 16), count)

        def send(link, slot):
            sx, sy, items = LINKS[link]
            src = first if due(link, slot) < SPLIT[c] else full
            for piece, (lo, count) in enumerate(PIECES[slot]):
                rows = rows_of(*items[slot], lo, count)
                pltpu.make_async_remote_copy(
                    src_ref=src.at[rows], dst_ref=full.at[rows], send_sem=send_sem,
                    recv_sem=recv_sem.at[FLAG[slot] - FLAG[min(SPLIT)] + piece],
                    device_id=device(sx, sy, c), device_id_type=MESH,
                ).start()

        def share(src, dx, dy, q, lo=0, count=UNIT):
            rows = rows_of(dx, dy, q, lo, count)
            pltpu.make_async_remote_copy(
                src_ref=src.at[rows], dst_ref=full.at[rows], send_sem=send_sem,
                recv_sem=pair_recv, device_id=device(0, 0, 1 - c), device_id_type=MESH,
            ).start()

        sent = [SPLIT[c]] * 4
        held = [(first, *received(link, slot)) for slot in range(min(SPLIT), SPLIT[c]) for link in range(4)]
        for slot in range(SPLIT[c] - 1, STEPS):
            if c == FIRST and slot == READY:
                pl.semaphore_wait(ready, 1)
            for piece, (lo, count) in enumerate(PIECES[slot] if slot >= SPLIT[c] else ()):
                four = pl.ds(0, 4 * count)
                pltpu.make_async_copy(
                    full.at[four], full.at[four], recv_sem.at[FLAG[slot] - FLAG[min(SPLIT)] + piece]
                ).wait()
                for link in range(4):
                    item = (full, *received(link, slot), lo, count)
                    if c == FIRST and slot < READY:
                        held.append(item)
                    else:
                        share(*item)
            for link in range(4):
                while sent[link] < STEPS and due(link, sent[link]) <= slot:
                    send(link, sent[link])
                    sent[link] += 1
            if c != FIRST or slot >= READY:
                for _ in range(min(PACE, len(held))):
                    share(*held.pop(0))
        assert not held
        other = pl.ds(0, 4 * (STEPS - min(SPLIT)) * UNIT)
        pltpu.make_async_copy(full.at[other], full.at[other], pair_recv).wait()
        everything = pl.ds(0, (4 * (STEPS - SPLIT[c]) + 4 * (STEPS - min(SPLIT))) * UNIT)
        pltpu.make_async_copy(full.at[everything], full.at[everything], send_sem).wait()

    for c in range(NC):
        pl.when(core == c)(functools.partial(run, c))


def write_units(full, query, key, value, sem, first):
    me = lax.axis_index("rows")
    core = lax.rem(me, NC)
    chip = lax.div(me, NC)
    x = lax.rem(chip, NX)
    y = lax.div(chip, NX)

    def run(c):
        count = 0
        for net in range(NC):
            units = [(0, 0, q) for q in range(4)] if first else []
            last = SPLIT[c] if net == c else min(SPLIT)
            for slot in range(0, last) if first else range(last, STEPS):
                units += [received(link, slot) for link in range(4)]
            for dx, dy, q in units:
                chip = lax.rem(y + dy % NY, NY) * NX + lax.rem(x + dx % NX, NX)
                src = pl.ds(pl.multiple_of((net * NX * NY + chip) * 256 + q * UNIT, UNIT), UNIT)
                dst = pl.multiple_of((chip * NC + net) * 256, 256)
                pltpu.make_async_copy(
                    full.at[src, pl.ds(0, 1024)], query.at[pl.ds(pl.multiple_of(dst + q * UNIT, UNIT), UNIT)], sem
                ).start()
                pltpu.make_async_copy(
                    full.at[src, pl.ds(1024, 128)],
                    (key, value)[q % 2].at[:, pl.ds(pl.multiple_of(dst + 128 * (q // 2), 128), 128)],
                    sem,
                ).start()
            count += len(units)
        everything = pl.ds(0, count * UNIT)
        pltpu.make_async_copy(full.at[everything], full.at[everything], sem).wait()

    for c in range(NC):
        pl.when(core == c)(functools.partial(run, c))


def write_first(full, total, query, key, value, scale_q, scale_k, scale_v, token, near_k, near_v, sem):
    near_k[...] = total[:, 1024:1088]
    near_v[...] = total[:, 1088:1152]
    thin = [
        pltpu.make_async_copy(total.at[:, pl.ds(0, 1024)], scale_q, sem.at[1]),
        pltpu.make_async_copy(near_k, scale_k, sem.at[2]),
        pltpu.make_async_copy(near_v, scale_v, sem.at[3]),
    ]
    for copy in thin:
        copy.start()
    token[...] = jnp.zeros_like(token)
    write_units(full, query, key, value, sem.at[0], True)
    for copy in thin:
        copy.wait()


def write_rest(full, query_in, key_in, value_in, query, key, value, sem):
    write_units(full, query, key, value, sem.at[0], False)


def local(one_query, other_query, one_key, other_key, one_value, other_value, mix_share, norm_gain):
    hbm = pl.BlockSpec(memory_space=pltpu.HBM)
    vmem = pl.BlockSpec(memory_space=pltpu.VMEM)
    f32, bf16 = jnp.float32, jnp.bfloat16
    first, total = pl.pallas_call(
        gather_kernel,
        out_shape=(pltpu.VMEM((8192, 1152), bf16), pltpu.VMEM((1, 1152), f32)),
        in_specs=[hbm] * 8,
        out_specs=(vmem, vmem),
        scratch_shapes=[
            pltpu.VMEM((2, 256, 1024), f32),
            pltpu.VMEM((2, 128, 256), f32),
            pltpu.VMEM((2, 1, 256), f32),
            pltpu.VMEM((256, 1152), f32),
            pltpu.VMEM((1, 1152), f32),
            pltpu.VMEM((8, 1, 1152), f32),
            pltpu.VMEM((1, 1152), f32),
            pltpu.VMEM((4, 1, 1152), f32),
            pltpu.VMEM((4, UNIT, 1152), f32),
            pltpu.SemaphoreType.DMA((4,)),
            pltpu.SemaphoreType.DMA((2,)),
            pltpu.SemaphoreType.DMA((2,)),
            pltpu.SemaphoreType.DMA,
            pltpu.SemaphoreType.DMA,
            pltpu.SemaphoreType.DMA,
            pltpu.SemaphoreType.DMA((max(SPLIT),)),
            pltpu.SemaphoreType.DMA,
        ],
        compiler_params=pltpu.CompilerParams(
            collective_id=0, has_side_effects=True, vmem_limit_bytes=10 * 2**20
        ),
        name="gather",
    )(*(
        pltpu.with_memory_space_constraint(a, pltpu.HBM)
        for a in (
            one_query, other_query, one_key.T, other_key.T, one_value.T, other_value.T,
            mix_share.reshape(1, 256), norm_gain.reshape(1, 256),
        )
    ))
    placed = (
        jax.ShapeDtypeStruct((8192, 1024), bf16),
        jax.ShapeDtypeStruct((64, 8192), bf16),
        jax.ShapeDtypeStruct((64, 8192), bf16),
    )
    query, key, value, scale_q, scale_k, scale_v, token = pl.pallas_call(
        write_first,
        out_shape=placed + (
            jax.ShapeDtypeStruct((1, 1024), f32),
            jax.ShapeDtypeStruct((1, 64), f32),
            jax.ShapeDtypeStruct((1, 64), f32),
            pltpu.VMEM((8, 128), f32),
        ),
        in_specs=[vmem, vmem],
        out_specs=[hbm] * 6 + [vmem],
        scratch_shapes=[pltpu.VMEM((1, 64), f32), pltpu.VMEM((1, 64), f32), pltpu.SemaphoreType.DMA((4,))],
        compiler_params=pltpu.CompilerParams(vmem_limit_bytes=2 * 2**20),
        name="write_first",
    )(first, total)
    rest = pl.pallas_call(
        rest_kernel,
        out_shape=pltpu.VMEM((8192, 1152), bf16),
        in_specs=[vmem, vmem],
        out_specs=vmem,
        scratch_shapes=[
            pltpu.SemaphoreType.DMA,
            pltpu.SemaphoreType.DMA((FLAG[STEPS] - FLAG[min(SPLIT)],)),
            pltpu.SemaphoreType.DMA,
            pltpu.SemaphoreType.REGULAR,
        ],
        compiler_params=pltpu.CompilerParams(collective_id=1, has_side_effects=True, vmem_limit_bytes=2 * 2**20),
        name="rest",
    )(first, token)
    query, key, value = pl.pallas_call(
        write_rest,
        out_shape=placed,
        in_specs=[vmem, hbm, hbm, hbm],
        out_specs=[hbm] * 3,
        input_output_aliases={1: 0, 2: 1, 3: 2},
        scratch_shapes=[pltpu.SemaphoreType.DMA((1,))],
        compiler_params=pltpu.CompilerParams(vmem_limit_bytes=2 * 2**20),
        name="write_rest",
    )(rest, query, key, value)
    return (query, key.T, value.T, scale_q.reshape(1024), scale_k.reshape(64), scale_v.reshape(64))


def solution(mesh):
    return jax.shard_map(
        local,
        mesh=mesh,
        in_specs=(
            P("rows", "cols"),
            P("rows", "cols"),
            P("rows", "cols"),
            P("rows", "cols"),
            P("rows", "cols"),
            P("rows", "cols"),
            P("rows"),
            P("rows"),
        ),
        out_specs=(
            P(None, "cols"),
            P(None, "cols"),
            P(None, "cols"),
            P("cols"),
            P("cols"),
            P("cols"),
        ),
        check_vma=False,
    )
```

```python
import functools

import jax
import jax.numpy as jnp
from jax import lax
from jax.experimental import pallas as pl
from jax.experimental.pallas import tpu as pltpu
from jax.sharding import PartitionSpec as P

D_MODEL = 8192
MESH = pl.DeviceIdType.MESH
NX, NY, NC = 4, 4, 2
UNIT = 64

PLUS_X = (
    (0, 0, 0), (0, 0, 1), (0, 0, 2), (-1, 0, 0), (0, 0, 3), (0, -1, 2), (0, 1, 2), (-1, 0, 2),
    (0, 2, 2), (-1, -1, 2), (0, -1, 3), (-1, 1, 2), (0, 1, 3), (-1, 2, 2), (0, 2, 3),
)


def mirrored(items):
    return tuple((-dx, -dy, q ^ 1) for dx, dy, q in items)


def turned(items):
    return tuple((dy, dx, q ^ 2) for dx, dy, q in items)


LINKS = (
    (1, 0, PLUS_X),
    (-1, 0, mirrored(PLUS_X)),
    (0, 1, turned(PLUS_X)),
    (0, -1, mirrored(turned(PLUS_X))),
)


def received(link, slot):
    sx, sy, items = LINKS[link]
    dx, dy, q = items[slot]
    return ((dx - sx) % NX, (dy - sy) % NY, q)


STEPS = len(PLUS_X)
PIECES = [((0, UNIT),)] * (STEPS - 1) + [((0, 32), (32, 16), (48, 16))]
FLAG = [sum(len(p) for p in PIECES[1:slot]) for slot in range(STEPS + 1)]
SPLIT = (6, 13)
READY = 11
PACE = 40
FIRST = SPLIT.index(min(SPLIT))
EARLY = ((0, 32), (32, 32))
ARRIVAL = {received(link, slot): slot for link in range(4) for slot in range(STEPS)}


def due(link, slot):
    dx, dy, q = LINKS[link][2][slot]
    return -1 if (dx, dy) == (0, 0) else ARRIVAL[(dx % NX, dy % NY, q)]


def gather_kernel(
    one_q, other_q, one_k, other_k, one_v, other_v, mix, gain,
    full, total,
    in_q, in_kv, in_vec,
    gained, part, row_sums, mid, col_sums, early_in,
    load_sem, sum_send, sum_recv, early_send, early_recv, send_sem, recv_sem, pair_recv,
):
    me = lax.axis_index("rows")
    core = lax.rem(me, NC)
    chip = lax.div(me, NC)
    x = lax.rem(chip, NX)
    y = lax.div(chip, NX)

    def at(dx, dy):
        return lax.rem(y + dy % NY, NY) * NX + lax.rem(x + dx % NX, NX)

    def device(dx, dy, c):
        return {"rows": at(dx, dy) * NC + c}

    row_peers = [(2, 0, core), (2, 0, 1 - core), (1, 0, core), (3, 0, core), (1, 0, 1 - core), (3, 0, 1 - core), (0, 0, 1 - core)]
    col_peers = [(0, 2, core), (0, 1, core), (0, 3, core)]
    small = [
        pltpu.make_async_copy(mix, in_vec.at[0], load_sem.at[0]),
        pltpu.make_async_copy(gain, in_vec.at[1], load_sem.at[0]),
    ]
    thin = [
        pltpu.make_async_copy(one_k, in_kv.at[0, pl.ds(0, 64)], load_sem.at[1]),
        pltpu.make_async_copy(one_v, in_kv.at[0, pl.ds(64, 64)], load_sem.at[1]),
        pltpu.make_async_copy(other_k, in_kv.at[1, pl.ds(0, 64)], load_sem.at[1]),
        pltpu.make_async_copy(other_v, in_kv.at[1, pl.ds(64, 64)], load_sem.at[1]),
    ]
    wide = []
    for h in range(2):
        rows = pl.ds(128 * h, 128)
        wide.append(pltpu.make_async_copy(one_q.at[rows], in_q.at[0, rows], load_sem.at[2 + h]))
        wide.append(pltpu.make_async_copy(other_q.at[rows], in_q.at[1, rows], load_sem.at[2 + h]))
    for copy in small + thin + wide:
        copy.start()
    barrier = pltpu.get_barrier_semaphore()
    for peer in row_peers + col_peers:
        pl.semaphore_signal(barrier, inc=1, device_id=device(*peer), device_id_type=MESH)
    pltpu.make_async_copy(in_vec, in_vec, load_sem.at[0]).wait()
    pltpu.make_async_copy(in_kv, in_kv, load_sem.at[1]).wait()

    m, g = in_vec[0], in_vec[1]
    kv = (m * in_kv[0] + (1.0 - m) * in_kv[1]) * g
    kv_sum = jnp.sum(jnp.abs(kv), axis=1, keepdims=True)
    gained[pl.ds(0, 128), pl.ds(1024, 128)] = kv[:, :128]
    gained[pl.ds(128, 128), pl.ds(1024, 128)] = kv[:, 128:]
    part[:, pl.ds(1024, 128)] = jnp.transpose(jnp.broadcast_to(kv_sum, (128, 128)))[:1]

    sums = jnp.zeros((8, 1024), jnp.float32)
    for h in range(2):
        half = in_q.at[:, pl.ds(128 * h, 128)]
        pltpu.make_async_copy(half, half, load_sem.at[2 + h]).wait()
        m_rows = jnp.transpose(jnp.broadcast_to(m[:, 128 * h : 128 * h + 128], (128, 128)))
        g_rows = jnp.transpose(jnp.broadcast_to(g[:, 128 * h : 128 * h + 128], (128, 128)))
        for t in range(16):
            rows = pl.ds(128 * h + 8 * t, 8)
            mt = jnp.concatenate([m_rows[8 * t : 8 * t + 8]] * 8, axis=1)
            gt = jnp.concatenate([g_rows[8 * t : 8 * t + 8]] * 8, axis=1)
            value = (mt * in_q[0, rows, :] + (1.0 - mt) * in_q[1, rows, :]) * gt
            gained[rows, pl.ds(0, 1024)] = value
            sums = sums + jnp.abs(value)
    part[:, pl.ds(0, 1024)] = jnp.sum(sums, axis=0, keepdims=True)

    pl.semaphore_wait(barrier, len(row_peers) + len(col_peers))
    def early(link, lo, count):
        sx, sy, items = LINKS[link]
        pltpu.make_async_remote_copy(
            src_ref=gained.at[pl.ds(items[0][2] * UNIT + lo, count)], dst_ref=early_in.at[link, pl.ds(lo, count)],
            send_sem=early_send, recv_sem=early_recv, device_id=device(sx, sy, core), device_id_type=MESH,
        ).start()

    own = x * NC + core
    for dx, dy, c in row_peers:
        pltpu.make_async_remote_copy(
            src_ref=part, dst_ref=row_sums.at[own], send_sem=sum_send.at[0],
            recv_sem=sum_recv.at[0], device_id=device(dx, dy, c), device_id_type=MESH,
        ).start()
    for link in (0, 1):
        early(link, 0, UNIT)
    for link in (2, 3):
        early(link, *EARLY[0])
    row_sums[own] = part[...]
    others = row_sums.at[pl.ds(0, len(row_peers))]
    pltpu.make_async_copy(others, others, sum_recv.at[0]).wait()
    subtotal = row_sums[0]
    for i in range(1, NX * NC):
        subtotal = subtotal + row_sums[i]
    mid[...] = subtotal
    for dx, dy, c in col_peers:
        pltpu.make_async_remote_copy(
            src_ref=mid, dst_ref=col_sums.at[y], send_sem=sum_send.at[1],
            recv_sem=sum_recv.at[1], device_id=device(dx, dy, c), device_id_type=MESH,
        ).start()
    for link in (2, 3):
        early(link, *EARLY[1])
    col_sums[y] = mid[...]
    others = col_sums.at[pl.ds(0, len(col_peers))]
    pltpu.make_async_copy(others, others, sum_recv.at[1]).wait()
    subtotal = col_sums[0]
    for i in range(1, NY):
        subtotal = subtotal + col_sums[i]
    scale = subtotal / D_MODEL
    total[...] = scale
    inverse = 1.0 / scale
    inverse_kv = jnp.transpose(jnp.broadcast_to(inverse[:, 1024:], (128, 128)))

    def rows_of(dx, dy, q):
        return pl.ds(pl.multiple_of((core * NX * NY + at(dx, dy)) * 256 + q * UNIT, UNIT), UNIT)

    def send(link, slot):
        sx, sy, items = LINKS[link]
        rows = rows_of(*items[slot])
        pltpu.make_async_remote_copy(
            src_ref=full.at[rows], dst_ref=full.at[rows], send_sem=send_sem,
            recv_sem=recv_sem.at[slot], device_id=device(sx, sy, core), device_id_type=MESH,
        ).start()

    def share(dx, dy, q):
        rows = rows_of(dx, dy, q)
        pltpu.make_async_remote_copy(
            src_ref=full.at[rows], dst_ref=full.at[rows], send_sem=send_sem,
            recv_sem=pair_recv, device_id=device(0, 0, 1 - core), device_id_type=MESH,
        ).start()

    def finish(dst, q, value):
        half = (q % 2) * UNIT
        full[dst, pl.ds(0, 1024)] = (value[:, :1024] * inverse[:, :1024]).astype(jnp.bfloat16)
        full[dst, pl.ds(1024, 128)] = (value[:, 1024:] * inverse_kv[half : half + UNIT]).astype(jnp.bfloat16)

    for q in range(4):
        finish(rows_of(0, 0, q), q, gained[pl.ds(q * UNIT, UNIT), :])

    def run(c):
        sent = [1, 1, 1, 1]
        for slot in range(-1, SPLIT[c]):
            if slot == 0:
                pltpu.make_async_copy(early_in, early_in, early_recv).wait()
                for link in range(4):
                    dx, dy, q = received(link, slot)
                    finish(rows_of(dx, dy, q), q, early_in[link])
                    share(dx, dy, q)
            elif slot > 0:
                four = pl.ds(0, 4 * UNIT)
                pltpu.make_async_copy(full.at[four], full.at[four], recv_sem.at[slot]).wait()
                if slot < min(SPLIT):
                    for link in range(4):
                        share(*received(link, slot))
            for link in range(4):
                while sent[link] < SPLIT[c] and due(link, sent[link]) <= slot:
                    send(link, sent[link])
                    sent[link] += 1
            if slot == -1:
                for q in range(4):
                    share(0, 0, q)
        other = pl.ds(0, (4 + 4 * min(SPLIT)) * UNIT)
        pltpu.make_async_copy(full.at[other], full.at[other], pair_recv).wait()
        everything = pl.ds(0, (4 * (SPLIT[c] - 1) + 4 + 4 * min(SPLIT)) * UNIT)
        pltpu.make_async_copy(full.at[everything], full.at[everything], send_sem).wait()

    for c in range(NC):
        pl.when(core == c)(functools.partial(run, c))
    pltpu.make_async_copy(gained, gained, early_send).wait()
    sums_sent = row_sums.at[pl.ds(0, len(row_peers))]
    pltpu.make_async_copy(sums_sent, sums_sent, sum_send.at[0]).wait()
    sums_sent = col_sums.at[pl.ds(0, len(col_peers))]
    pltpu.make_async_copy(sums_sent, sums_sent, sum_send.at[1]).wait()


def rest_kernel(first, token, full, send_sem, recv_sem, pair_recv, ready):
    me = lax.axis_index("rows")
    core = lax.rem(me, NC)
    chip = lax.div(me, NC)
    x = lax.rem(chip, NX)
    y = lax.div(chip, NX)

    def at(dx, dy):
        return lax.rem(y + dy % NY, NY) * NX + lax.rem(x + dx % NX, NX)

    def device(dx, dy, c):
        return {"rows": at(dx, dy) * NC + c}

    barrier = pltpu.get_barrier_semaphore()
    for sx, sy, _ in LINKS:
        pl.semaphore_signal(barrier, inc=1, device_id=device(sx, sy, core), device_id_type=MESH)

    def run(c):
        if c == FIRST:
            pl.semaphore_signal(barrier, inc=1, device_id=device(0, 0, 1 - FIRST), device_id_type=MESH)
        pl.semaphore_wait(barrier, 4 if c == FIRST else 5)
        if c != FIRST:
            pl.semaphore_signal(ready, inc=1, device_id=device(0, 0, FIRST), device_id_type=MESH)

        def rows_of(dx, dy, q, lo=0, count=UNIT):
            return pl.ds(pl.multiple_of((c * NX * NY + at(dx, dy)) * 256 + q * UNIT + lo, 16), count)

        def send(link, slot):
            sx, sy, items = LINKS[link]
            src = first if due(link, slot) < SPLIT[c] else full
            for piece, (lo, count) in enumerate(PIECES[slot]):
                rows = rows_of(*items[slot], lo, count)
                pltpu.make_async_remote_copy(
                    src_ref=src.at[rows], dst_ref=full.at[rows], send_sem=send_sem,
                    recv_sem=recv_sem.at[FLAG[slot] - FLAG[min(SPLIT)] + piece],
                    device_id=device(sx, sy, c), device_id_type=MESH,
                ).start()

        def share(src, dx, dy, q, lo=0, count=UNIT):
            rows = rows_of(dx, dy, q, lo, count)
            pltpu.make_async_remote_copy(
                src_ref=src.at[rows], dst_ref=full.at[rows], send_sem=send_sem,
                recv_sem=pair_recv, device_id=device(0, 0, 1 - c), device_id_type=MESH,
            ).start()

        sent = [SPLIT[c]] * 4
        held = [(first, *received(link, slot)) for slot in range(min(SPLIT), SPLIT[c]) for link in range(4)]
        for slot in range(SPLIT[c] - 1, STEPS):
            if c == FIRST and slot == READY:
                pl.semaphore_wait(ready, 1)
            for piece, (lo, count) in enumerate(PIECES[slot] if slot >= SPLIT[c] else ()):
                four = pl.ds(0, 4 * count)
                pltpu.make_async_copy(
                    full.at[four], full.at[four], recv_sem.at[FLAG[slot] - FLAG[min(SPLIT)] + piece]
                ).wait()
                for link in range(4):
                    item = (full, *received(link, slot), lo, count)
                    if c == FIRST and slot < READY:
                        held.append(item)
                    else:
                        share(*item)
            for link in range(4):
                while sent[link] < STEPS and due(link, sent[link]) <= slot:
                    send(link, sent[link])
                    sent[link] += 1
            if c != FIRST or slot >= READY:
                for _ in range(min(PACE, len(held))):
                    share(*held.pop(0))
        assert not held
        other = pl.ds(0, 4 * (STEPS - min(SPLIT)) * UNIT)
        pltpu.make_async_copy(full.at[other], full.at[other], pair_recv).wait()
        everything = pl.ds(0, (4 * (STEPS - SPLIT[c]) + 4 * (STEPS - min(SPLIT))) * UNIT)
        pltpu.make_async_copy(full.at[everything], full.at[everything], send_sem).wait()

    for c in range(NC):
        pl.when(core == c)(functools.partial(run, c))


def write_units(full, query, key, value, sem, first):
    me = lax.axis_index("rows")
    core = lax.rem(me, NC)
    chip = lax.div(me, NC)
    x = lax.rem(chip, NX)
    y = lax.div(chip, NX)

    def run(c):
        count = 0
        for net in range(NC):
            units = [(0, 0, q) for q in range(4)] if first else []
            last = SPLIT[c] if net == c else min(SPLIT)
            for slot in range(0, last) if first else range(last, STEPS):
                units += [received(link, slot) for link in range(4)]
            for dx, dy, q in units:
                chip = lax.rem(y + dy % NY, NY) * NX + lax.rem(x + dx % NX, NX)
                src = pl.ds(pl.multiple_of((net * NX * NY + chip) * 256 + q * UNIT, UNIT), UNIT)
                dst = pl.multiple_of((chip * NC + net) * 256, 256)
                pltpu.make_async_copy(
                    full.at[src, pl.ds(0, 1024)], query.at[pl.ds(pl.multiple_of(dst + q * UNIT, UNIT), UNIT)], sem
                ).start()
                pltpu.make_async_copy(
                    full.at[src, pl.ds(1024, 128)],
                    (key, value)[q % 2].at[:, pl.ds(pl.multiple_of(dst + 128 * (q // 2), 128), 128)],
                    sem,
                ).start()
            count += len(units)
        everything = pl.ds(0, count * UNIT)
        pltpu.make_async_copy(full.at[everything], full.at[everything], sem).wait()

    for c in range(NC):
        pl.when(core == c)(functools.partial(run, c))


def write_first(full, total, query, key, value, scale_q, scale_k, scale_v, token, near_k, near_v, sem):
    near_k[...] = total[:, 1024:1088]
    near_v[...] = total[:, 1088:1152]
    thin = [
        pltpu.make_async_copy(total.at[:, pl.ds(0, 1024)], scale_q, sem.at[1]),
        pltpu.make_async_copy(near_k, scale_k, sem.at[2]),
        pltpu.make_async_copy(near_v, scale_v, sem.at[3]),
    ]
    for copy in thin:
        copy.start()
    token[...] = jnp.zeros_like(token)
    write_units(full, query, key, value, sem.at[0], True)
    for copy in thin:
        copy.wait()


def write_rest(full, query_in, key_in, value_in, query, key, value, sem):
    write_units(full, query, key, value, sem.at[0], False)


def local(one_query, other_query, one_key, other_key, one_value, other_value, mix_share, norm_gain):
    hbm = pl.BlockSpec(memory_space=pltpu.HBM)
    vmem = pl.BlockSpec(memory_space=pltpu.VMEM)
    f32, bf16 = jnp.float32, jnp.bfloat16
    first, total = pl.pallas_call(
        gather_kernel,
        out_shape=(pltpu.VMEM((8192, 1152), bf16), pltpu.VMEM((1, 1152), f32)),
        in_specs=[hbm] * 8,
        out_specs=(vmem, vmem),
        scratch_shapes=[
            pltpu.VMEM((2, 256, 1024), f32),
            pltpu.VMEM((2, 128, 256), f32),
            pltpu.VMEM((2, 1, 256), f32),
            pltpu.VMEM((256, 1152), f32),
            pltpu.VMEM((1, 1152), f32),
            pltpu.VMEM((8, 1, 1152), f32),
            pltpu.VMEM((1, 1152), f32),
            pltpu.VMEM((4, 1, 1152), f32),
            pltpu.VMEM((4, UNIT, 1152), f32),
            pltpu.SemaphoreType.DMA((4,)),
            pltpu.SemaphoreType.DMA((2,)),
            pltpu.SemaphoreType.DMA((2,)),
            pltpu.SemaphoreType.DMA,
            pltpu.SemaphoreType.DMA,
            pltpu.SemaphoreType.DMA,
            pltpu.SemaphoreType.DMA((max(SPLIT),)),
            pltpu.SemaphoreType.DMA,
        ],
        compiler_params=pltpu.CompilerParams(
            collective_id=0, has_side_effects=True, vmem_limit_bytes=10 * 2**20
        ),
        name="gather",
    )(*(
        pltpu.with_memory_space_constraint(a, pltpu.HBM)
        for a in (
            one_query, other_query, one_key.T, other_key.T, one_value.T, other_value.T,
            mix_share.reshape(1, 256), norm_gain.reshape(1, 256),
        )
    ))
    placed = (
        jax.ShapeDtypeStruct((8192, 1024), bf16),
        jax.ShapeDtypeStruct((64, 8192), bf16),
        jax.ShapeDtypeStruct((64, 8192), bf16),
    )
    query, key, value, scale_q, scale_k, scale_v, token = pl.pallas_call(
        write_first,
        out_shape=placed + (
            jax.ShapeDtypeStruct((1, 1024), f32),
            jax.ShapeDtypeStruct((1, 64), f32),
            jax.ShapeDtypeStruct((1, 64), f32),
            pltpu.VMEM((8, 128), f32),
        ),
        in_specs=[vmem, vmem],
        out_specs=[hbm] * 6 + [vmem],
        scratch_shapes=[pltpu.VMEM((1, 64), f32), pltpu.VMEM((1, 64), f32), pltpu.SemaphoreType.DMA((4,))],
        compiler_params=pltpu.CompilerParams(vmem_limit_bytes=2 * 2**20),
        name="write_first",
    )(first, total)
    rest = pl.pallas_call(
        rest_kernel,
        out_shape=pltpu.VMEM((8192, 1152), bf16),
        in_specs=[vmem, vmem],
        out_specs=vmem,
        scratch_shapes=[
            pltpu.SemaphoreType.DMA,
            pltpu.SemaphoreType.DMA((FLAG[STEPS] - FLAG[min(SPLIT)],)),
            pltpu.SemaphoreType.DMA,
            pltpu.SemaphoreType.REGULAR,
        ],
        compiler_params=pltpu.CompilerParams(collective_id=1, has_side_effects=True, vmem_limit_bytes=2 * 2**20),
        name="rest",
    )(first, token)
    query, key, value = pl.pallas_call(
        write_rest,
        out_shape=placed,
        in_specs=[vmem, hbm, hbm, hbm],
        out_specs=[hbm] * 3,
        input_output_aliases={1: 0, 2: 1, 3: 2},
        scratch_shapes=[pltpu.SemaphoreType.DMA((1,))],
        compiler_params=pltpu.CompilerParams(vmem_limit_bytes=2 * 2**20),
        name="write_rest",
    )(rest, query, key, value)
    return (query, key.T, value.T, scale_q.reshape(1024), scale_k.reshape(64), scale_v.reshape(64))


def solution(mesh):
    return jax.shard_map(
        local,
        mesh=mesh,
        in_specs=(
            P("rows", "cols"),
            P("rows", "cols"),
            P("rows", "cols"),
            P("rows", "cols"),
            P("rows", "cols"),
            P("rows", "cols"),
            P("rows"),
            P("rows"),
        ),
        out_specs=(
            P(None, "cols"),
            P(None, "cols"),
            P(None, "cols"),
            P("cols"),
            P("cols"),
            P("cols"),
        ),
        check_vma=False,
    )
```

```python
import functools

import jax
import jax.numpy as jnp
from jax import lax
from jax.experimental import pallas as pl
from jax.experimental.pallas import tpu as pltpu
from jax.sharding import PartitionSpec as P

D_MODEL = 8192
MESH = pl.DeviceIdType.MESH
NX, NY, NC = 4, 4, 2
UNIT = 64

PLUS_X = (
    (0, 0, 0), (0, 0, 1), (0, 0, 2), (-1, 0, 0), (0, 0, 3), (0, -1, 2), (0, 1, 2), (-1, 0, 2),
    (0, 2, 2), (-1, -1, 2), (0, -1, 3), (-1, 1, 2), (0, 1, 3), (-1, 2, 2), (0, 2, 3),
)


def mirrored(items):
    return tuple((-dx, -dy, q ^ 1) for dx, dy, q in items)


def turned(items):
    return tuple((dy, dx, q ^ 2) for dx, dy, q in items)


LINKS = (
    (1, 0, PLUS_X),
    (-1, 0, mirrored(PLUS_X)),
    (0, 1, turned(PLUS_X)),
    (0, -1, mirrored(turned(PLUS_X))),
)


def received(link, slot):
    sx, sy, items = LINKS[link]
    dx, dy, q = items[slot]
    return ((dx - sx) % NX, (dy - sy) % NY, q)


STEPS = len(PLUS_X)
PIECES = [((0, UNIT),)] * (STEPS - 1) + [((0, 32), (32, 16), (48, 16))]
FLAG = [sum(len(p) for p in PIECES[1:slot]) for slot in range(STEPS + 1)]
SPLIT = (7, 13)
READY = 11
PACE = 40
FIRST = SPLIT.index(min(SPLIT))
SHARED = min(SPLIT) - 1
EARLY = ((0, 32), (32, 32))
ARRIVAL = {received(link, slot): slot for link in range(4) for slot in range(STEPS)}


def due(link, slot):
    dx, dy, q = LINKS[link][2][slot]
    return -1 if (dx, dy) == (0, 0) else ARRIVAL[(dx % NX, dy % NY, q)]


def gather_kernel(
    one_q, other_q, one_k, other_k, one_v, other_v, mix, gain,
    full, total,
    in_q, in_kv, in_vec,
    gained, part, row_sums, mid, col_sums, early_in,
    load_sem, sum_send, sum_recv, early_send, early_recv, send_sem, recv_sem, pair_recv,
):
    me = lax.axis_index("rows")
    core = lax.rem(me, NC)
    chip = lax.div(me, NC)
    x = lax.rem(chip, NX)
    y = lax.div(chip, NX)

    def at(dx, dy):
        return lax.rem(y + dy % NY, NY) * NX + lax.rem(x + dx % NX, NX)

    def device(dx, dy, c):
        return {"rows": at(dx, dy) * NC + c}

    row_peers = [(2, 0, core), (2, 0, 1 - core), (1, 0, core), (3, 0, core), (1, 0, 1 - core), (3, 0, 1 - core), (0, 0, 1 - core)]
    col_peers = [(0, 2, core), (0, 1, core), (0, 3, core)]
    small = [
        pltpu.make_async_copy(mix, in_vec.at[0], load_sem.at[0]),
        pltpu.make_async_copy(gain, in_vec.at[1], load_sem.at[0]),
    ]
    thin = [
        pltpu.make_async_copy(one_k, in_kv.at[0, pl.ds(0, 64)], load_sem.at[1]),
        pltpu.make_async_copy(one_v, in_kv.at[0, pl.ds(64, 64)], load_sem.at[1]),
        pltpu.make_async_copy(other_k, in_kv.at[1, pl.ds(0, 64)], load_sem.at[1]),
        pltpu.make_async_copy(other_v, in_kv.at[1, pl.ds(64, 64)], load_sem.at[1]),
    ]
    wide = []
    for h in range(2):
        rows = pl.ds(128 * h, 128)
        wide.append(pltpu.make_async_copy(one_q.at[rows], in_q.at[0, rows], load_sem.at[2 + h]))
        wide.append(pltpu.make_async_copy(other_q.at[rows], in_q.at[1, rows], load_sem.at[2 + h]))
    for copy in small + thin + wide:
        copy.start()
    barrier = pltpu.get_barrier_semaphore()
    for peer in row_peers + col_peers:
        pl.semaphore_signal(barrier, inc=1, device_id=device(*peer), device_id_type=MESH)
    pltpu.make_async_copy(in_vec, in_vec, load_sem.at[0]).wait()
    pltpu.make_async_copy(in_kv, in_kv, load_sem.at[1]).wait()

    m, g = in_vec[0], in_vec[1]
    kv = (m * in_kv[0] + (1.0 - m) * in_kv[1]) * g
    kv_sum = jnp.sum(jnp.abs(kv), axis=1, keepdims=True)
    gained[pl.ds(0, 128), pl.ds(1024, 128)] = kv[:, :128]
    gained[pl.ds(128, 128), pl.ds(1024, 128)] = kv[:, 128:]
    part[:, pl.ds(1024, 128)] = jnp.transpose(jnp.broadcast_to(kv_sum, (128, 128)))[:1]

    sums = jnp.zeros((8, 1024), jnp.float32)
    for h in range(2):
        half = in_q.at[:, pl.ds(128 * h, 128)]
        pltpu.make_async_copy(half, half, load_sem.at[2 + h]).wait()
        m_rows = jnp.transpose(jnp.broadcast_to(m[:, 128 * h : 128 * h + 128], (128, 128)))
        g_rows = jnp.transpose(jnp.broadcast_to(g[:, 128 * h : 128 * h + 128], (128, 128)))
        for t in range(16):
            rows = pl.ds(128 * h + 8 * t, 8)
            mt = jnp.concatenate([m_rows[8 * t : 8 * t + 8]] * 8, axis=1)
            gt = jnp.concatenate([g_rows[8 * t : 8 * t + 8]] * 8, axis=1)
            value = (mt * in_q[0, rows, :] + (1.0 - mt) * in_q[1, rows, :]) * gt
            gained[rows, pl.ds(0, 1024)] = value
            sums = sums + jnp.abs(value)
    part[:, pl.ds(0, 1024)] = jnp.sum(sums, axis=0, keepdims=True)

    pl.semaphore_wait(barrier, len(row_peers) + len(col_peers))
    def early(link, lo, count):
        sx, sy, items = LINKS[link]
        pltpu.make_async_remote_copy(
            src_ref=gained.at[pl.ds(items[0][2] * UNIT + lo, count)], dst_ref=early_in.at[link, pl.ds(lo, count)],
            send_sem=early_send, recv_sem=early_recv, device_id=device(sx, sy, core), device_id_type=MESH,
        ).start()

    own = x * NC + core
    for dx, dy, c in row_peers:
        pltpu.make_async_remote_copy(
            src_ref=part, dst_ref=row_sums.at[own], send_sem=sum_send.at[0],
            recv_sem=sum_recv.at[0], device_id=device(dx, dy, c), device_id_type=MESH,
        ).start()
    for link in (0, 1):
        early(link, 0, UNIT)
    for link in (2, 3):
        early(link, *EARLY[0])
    row_sums[own] = part[...]
    others = row_sums.at[pl.ds(0, len(row_peers))]
    pltpu.make_async_copy(others, others, sum_recv.at[0]).wait()
    subtotal = row_sums[0]
    for i in range(1, NX * NC):
        subtotal = subtotal + row_sums[i]
    mid[...] = subtotal
    for dx, dy, c in col_peers:
        pltpu.make_async_remote_copy(
            src_ref=mid, dst_ref=col_sums.at[y], send_sem=sum_send.at[1],
            recv_sem=sum_recv.at[1], device_id=device(dx, dy, c), device_id_type=MESH,
        ).start()
    for link in (2, 3):
        early(link, *EARLY[1])
    col_sums[y] = mid[...]
    others = col_sums.at[pl.ds(0, len(col_peers))]
    pltpu.make_async_copy(others, others, sum_recv.at[1]).wait()
    subtotal = col_sums[0]
    for i in range(1, NY):
        subtotal = subtotal + col_sums[i]
    scale = subtotal / D_MODEL
    total[...] = scale
    inverse = 1.0 / scale
    inverse_kv = jnp.transpose(jnp.broadcast_to(inverse[:, 1024:], (128, 128)))

    def rows_of(dx, dy, q):
        return pl.ds(pl.multiple_of((core * NX * NY + at(dx, dy)) * 256 + q * UNIT, UNIT), UNIT)

    def send(link, slot):
        sx, sy, items = LINKS[link]
        rows = rows_of(*items[slot])
        pltpu.make_async_remote_copy(
            src_ref=full.at[rows], dst_ref=full.at[rows], send_sem=send_sem,
            recv_sem=recv_sem.at[slot], device_id=device(sx, sy, core), device_id_type=MESH,
        ).start()

    def share(dx, dy, q):
        rows = rows_of(dx, dy, q)
        pltpu.make_async_remote_copy(
            src_ref=full.at[rows], dst_ref=full.at[rows], send_sem=send_sem,
            recv_sem=pair_recv, device_id=device(0, 0, 1 - core), device_id_type=MESH,
        ).start()

    def finish(dst, q, value):
        half = (q % 2) * UNIT
        full[dst, pl.ds(0, 1024)] = (value[:, :1024] * inverse[:, :1024]).astype(jnp.bfloat16)
        full[dst, pl.ds(1024, 128)] = (value[:, 1024:] * inverse_kv[half : half + UNIT]).astype(jnp.bfloat16)

    for q in range(4):
        finish(rows_of(0, 0, q), q, gained[pl.ds(q * UNIT, UNIT), :])

    def run(c):
        sent = [1, 1, 1, 1]
        for slot in range(-1, SPLIT[c]):
            if slot == 0:
                pltpu.make_async_copy(early_in, early_in, early_recv).wait()
                for link in range(4):
                    dx, dy, q = received(link, slot)
                    finish(rows_of(dx, dy, q), q, early_in[link])
                    share(dx, dy, q)
            elif slot > 0:
                four = pl.ds(0, 4 * UNIT)
                pltpu.make_async_copy(full.at[four], full.at[four], recv_sem.at[slot]).wait()
                if slot < SHARED:
                    for link in range(4):
                        share(*received(link, slot))
            for link in range(4):
                while sent[link] < SPLIT[c] and due(link, sent[link]) <= slot:
                    send(link, sent[link])
                    sent[link] += 1
            if slot == -1:
                for q in range(4):
                    share(0, 0, q)
        other = pl.ds(0, (4 + 4 * SHARED) * UNIT)
        pltpu.make_async_copy(full.at[other], full.at[other], pair_recv).wait()
        everything = pl.ds(0, (4 * (SPLIT[c] - 1) + 4 + 4 * SHARED) * UNIT)
        pltpu.make_async_copy(full.at[everything], full.at[everything], send_sem).wait()

    for c in range(NC):
        pl.when(core == c)(functools.partial(run, c))
    pltpu.make_async_copy(gained, gained, early_send).wait()
    sums_sent = row_sums.at[pl.ds(0, len(row_peers))]
    pltpu.make_async_copy(sums_sent, sums_sent, sum_send.at[0]).wait()
    sums_sent = col_sums.at[pl.ds(0, len(col_peers))]
    pltpu.make_async_copy(sums_sent, sums_sent, sum_send.at[1]).wait()


def rest_kernel(first, token, full, send_sem, recv_sem, pair_recv, ready):
    me = lax.axis_index("rows")
    core = lax.rem(me, NC)
    chip = lax.div(me, NC)
    x = lax.rem(chip, NX)
    y = lax.div(chip, NX)

    def at(dx, dy):
        return lax.rem(y + dy % NY, NY) * NX + lax.rem(x + dx % NX, NX)

    def device(dx, dy, c):
        return {"rows": at(dx, dy) * NC + c}

    barrier = pltpu.get_barrier_semaphore()
    for sx, sy, _ in LINKS:
        pl.semaphore_signal(barrier, inc=1, device_id=device(sx, sy, core), device_id_type=MESH)

    def run(c):
        if c == FIRST:
            pl.semaphore_signal(barrier, inc=1, device_id=device(0, 0, 1 - FIRST), device_id_type=MESH)
        pl.semaphore_wait(barrier, 4 if c == FIRST else 5)
        if c != FIRST:
            pl.semaphore_signal(ready, inc=1, device_id=device(0, 0, FIRST), device_id_type=MESH)

        def rows_of(dx, dy, q, lo=0, count=UNIT):
            return pl.ds(pl.multiple_of((c * NX * NY + at(dx, dy)) * 256 + q * UNIT + lo, 16), count)

        def send(link, slot):
            sx, sy, items = LINKS[link]
            src = first if due(link, slot) < SPLIT[c] else full
            for piece, (lo, count) in enumerate(PIECES[slot]):
                rows = rows_of(*items[slot], lo, count)
                pltpu.make_async_remote_copy(
                    src_ref=src.at[rows], dst_ref=full.at[rows], send_sem=send_sem,
                    recv_sem=recv_sem.at[FLAG[slot] - FLAG[min(SPLIT)] + piece],
                    device_id=device(sx, sy, c), device_id_type=MESH,
                ).start()

        def share(src, dx, dy, q, lo=0, count=UNIT):
            rows = rows_of(dx, dy, q, lo, count)
            pltpu.make_async_remote_copy(
                src_ref=src.at[rows], dst_ref=full.at[rows], send_sem=send_sem,
                recv_sem=pair_recv, device_id=device(0, 0, 1 - c), device_id_type=MESH,
            ).start()

        sent = [SPLIT[c]] * 4
        held = [(first, *received(link, slot)) for slot in range(SHARED, SPLIT[c]) for link in range(4)]
        for slot in range(SPLIT[c] - 1, STEPS):
            if c == FIRST and slot == READY:
                pl.semaphore_wait(ready, 1)
            for piece, (lo, count) in enumerate(PIECES[slot] if slot >= SPLIT[c] else ()):
                four = pl.ds(0, 4 * count)
                pltpu.make_async_copy(
                    full.at[four], full.at[four], recv_sem.at[FLAG[slot] - FLAG[min(SPLIT)] + piece]
                ).wait()
                for link in range(4):
                    item = (full, *received(link, slot), lo, count)
                    if c == FIRST and slot < READY:
                        held.append(item)
                    else:
                        share(*item)
            for link in range(4):
                while sent[link] < STEPS and due(link, sent[link]) <= slot:
                    send(link, sent[link])
                    sent[link] += 1
            if c != FIRST or slot >= READY:
                for _ in range(min(PACE, len(held))):
                    share(*held.pop(0))
        assert not held
        other = pl.ds(0, 4 * (STEPS - SHARED) * UNIT)
        pltpu.make_async_copy(full.at[other], full.at[other], pair_recv).wait()
        everything = pl.ds(0, (4 * (STEPS - SPLIT[c]) + 4 * (STEPS - SHARED)) * UNIT)
        pltpu.make_async_copy(full.at[everything], full.at[everything], send_sem).wait()

    for c in range(NC):
        pl.when(core == c)(functools.partial(run, c))


def write_units(full, query, key, value, sem, first):
    me = lax.axis_index("rows")
    core = lax.rem(me, NC)
    chip = lax.div(me, NC)
    x = lax.rem(chip, NX)
    y = lax.div(chip, NX)

    def run(c):
        count = 0
        for net in range(NC):
            units = [(0, 0, q) for q in range(4)] if first else []
            last = SPLIT[c] if net == c else SHARED
            for slot in range(0, last) if first else range(last, STEPS):
                units += [received(link, slot) for link in range(4)]
            for dx, dy, q in units:
                chip = lax.rem(y + dy % NY, NY) * NX + lax.rem(x + dx % NX, NX)
                src = pl.ds(pl.multiple_of((net * NX * NY + chip) * 256 + q * UNIT, UNIT), UNIT)
                dst = pl.multiple_of((chip * NC + net) * 256, 256)
                pltpu.make_async_copy(
                    full.at[src, pl.ds(0, 1024)], query.at[pl.ds(pl.multiple_of(dst + q * UNIT, UNIT), UNIT)], sem
                ).start()
                pltpu.make_async_copy(
                    full.at[src, pl.ds(1024, 128)],
                    (key, value)[q % 2].at[:, pl.ds(pl.multiple_of(dst + 128 * (q // 2), 128), 128)],
                    sem,
                ).start()
            count += len(units)
        everything = pl.ds(0, count * UNIT)
        pltpu.make_async_copy(full.at[everything], full.at[everything], sem).wait()

    for c in range(NC):
        pl.when(core == c)(functools.partial(run, c))


def write_first(full, total, query, key, value, scale_q, scale_k, scale_v, token, near_k, near_v, sem):
    near_k[...] = total[:, 1024:1088]
    near_v[...] = total[:, 1088:1152]
    thin = [
        pltpu.make_async_copy(total.at[:, pl.ds(0, 1024)], scale_q, sem.at[1]),
        pltpu.make_async_copy(near_k, scale_k, sem.at[2]),
        pltpu.make_async_copy(near_v, scale_v, sem.at[3]),
    ]
    for copy in thin:
        copy.start()
    token[...] = jnp.zeros_like(token)
    write_units(full, query, key, value, sem.at[0], True)
    for copy in thin:
        copy.wait()


def write_rest(full, query_in, key_in, value_in, query, key, value, sem):
    write_units(full, query, key, value, sem.at[0], False)


def local(one_query, other_query, one_key, other_key, one_value, other_value, mix_share, norm_gain):
    hbm = pl.BlockSpec(memory_space=pltpu.HBM)
    vmem = pl.BlockSpec(memory_space=pltpu.VMEM)
    f32, bf16 = jnp.float32, jnp.bfloat16
    first, total = pl.pallas_call(
        gather_kernel,
        out_shape=(pltpu.VMEM((8192, 1152), bf16), pltpu.VMEM((1, 1152), f32)),
        in_specs=[hbm] * 8,
        out_specs=(vmem, vmem),
        scratch_shapes=[
            pltpu.VMEM((2, 256, 1024), f32),
            pltpu.VMEM((2, 128, 256), f32),
            pltpu.VMEM((2, 1, 256), f32),
            pltpu.VMEM((256, 1152), f32),
            pltpu.VMEM((1, 1152), f32),
            pltpu.VMEM((8, 1, 1152), f32),
            pltpu.VMEM((1, 1152), f32),
            pltpu.VMEM((4, 1, 1152), f32),
            pltpu.VMEM((4, UNIT, 1152), f32),
            pltpu.SemaphoreType.DMA((4,)),
            pltpu.SemaphoreType.DMA((2,)),
            pltpu.SemaphoreType.DMA((2,)),
            pltpu.SemaphoreType.DMA,
            pltpu.SemaphoreType.DMA,
            pltpu.SemaphoreType.DMA,
            pltpu.SemaphoreType.DMA((max(SPLIT),)),
            pltpu.SemaphoreType.DMA,
        ],
        compiler_params=pltpu.CompilerParams(
            collective_id=0, has_side_effects=True, vmem_limit_bytes=10 * 2**20
        ),
        name="gather",
    )(*(
        pltpu.with_memory_space_constraint(a, pltpu.HBM)
        for a in (
            one_query, other_query, one_key.T, other_key.T, one_value.T, other_value.T,
            mix_share.reshape(1, 256), norm_gain.reshape(1, 256),
        )
    ))
    placed = (
        jax.ShapeDtypeStruct((8192, 1024), bf16),
        jax.ShapeDtypeStruct((64, 8192), bf16),
        jax.ShapeDtypeStruct((64, 8192), bf16),
    )
    query, key, value, scale_q, scale_k, scale_v, token = pl.pallas_call(
        write_first,
        out_shape=placed + (
            jax.ShapeDtypeStruct((1, 1024), f32),
            jax.ShapeDtypeStruct((1, 64), f32),
            jax.ShapeDtypeStruct((1, 64), f32),
            pltpu.VMEM((8, 128), f32),
        ),
        in_specs=[vmem, vmem],
        out_specs=[hbm] * 6 + [vmem],
        scratch_shapes=[pltpu.VMEM((1, 64), f32), pltpu.VMEM((1, 64), f32), pltpu.SemaphoreType.DMA((4,))],
        compiler_params=pltpu.CompilerParams(vmem_limit_bytes=2 * 2**20),
        name="write_first",
    )(first, total)
    rest = pl.pallas_call(
        rest_kernel,
        out_shape=pltpu.VMEM((8192, 1152), bf16),
        in_specs=[vmem, vmem],
        out_specs=vmem,
        scratch_shapes=[
            pltpu.SemaphoreType.DMA,
            pltpu.SemaphoreType.DMA((FLAG[STEPS] - FLAG[min(SPLIT)],)),
            pltpu.SemaphoreType.DMA,
            pltpu.SemaphoreType.REGULAR,
        ],
        compiler_params=pltpu.CompilerParams(collective_id=1, has_side_effects=True, vmem_limit_bytes=2 * 2**20),
        name="rest",
    )(first, token)
    query, key, value = pl.pallas_call(
        write_rest,
        out_shape=placed,
        in_specs=[vmem, hbm, hbm, hbm],
        out_specs=[hbm] * 3,
        input_output_aliases={1: 0, 2: 1, 3: 2},
        scratch_shapes=[pltpu.SemaphoreType.DMA((1,))],
        compiler_params=pltpu.CompilerParams(vmem_limit_bytes=2 * 2**20),
        name="write_rest",
    )(rest, query, key, value)
    return (query, key.T, value.T, scale_q.reshape(1024), scale_k.reshape(64), scale_v.reshape(64))


def solution(mesh):
    return jax.shard_map(
        local,
        mesh=mesh,
        in_specs=(
            P("rows", "cols"),
            P("rows", "cols"),
            P("rows", "cols"),
            P("rows", "cols"),
            P("rows", "cols"),
            P("rows", "cols"),
            P("rows"),
            P("rows"),
        ),
        out_specs=(
            P(None, "cols"),
            P(None, "cols"),
            P(None, "cols"),
            P("cols"),
            P("cols"),
            P("cols"),
        ),
        check_vma=False,
    )
```
